32 devices in a mesh: row: 4 (over x, core), col: 8 (over z, y).
Axes of the slice: x: 2, y: 2, z: 4, core: 2. Of those that a mesh axis runs over, the one named last changes fastest.
Arguments:
- counts: float32 [8192, 8192], P('row', 'col'), may hold values from 0 to 514, as said below
- labels: int32 [983040], replicated, may hold values from 0 to 8191, as said below
- edge_tiles: int32 [1024, 2, 128], P(('row', 'col')), may hold values from 0 to 983039, as said below
- proposals: int32 [2, 128], replicated, may hold values from 0 to 8191, as said below
- accept_flags: int32 [128], P('col'), may hold values 0 or 1
Outputs:
- count_matrix: float32 [8192, 8192], P('row', 'col')
- merge_cost: float32 [128], P('col')
- accepted_cost: float32 [128], P('col')
The draws below stay inside these ranges and needn't reach their ends.
Inputs may be any that keep to these rules, and one draw needn't show every extreme that they name: `counts`: Symmetric, whole numbers, every diagonal entry at least 2. `labels`: every block holds exactly 120 vertices. `edge_tiles`: each edge gives the two entries (label of its first vertex, label of its second) and the reverse; entry (r, s) lies in tile (r // 2048, s // 1024). Of the 8192 entries of one device's edges at most 576 lie in one tile, and in every draw some tile gets exactly 576 entries from every device. proposals[1, p] differs from proposals[0, p]; for p // 16 = c, proposals[0, p] lies in c * 1024 to (c + 1) * 1024 - 1, and these sources are distinct.
All inputs are finite; a program needn't handle non-finite values. No bound on the sum of `accept_flags` on one device may be relied on, other than what follows from the above.
Results may differ from the reference program's by a relative error of at most 0.0003.
Values sent between devices are 32-bit elements; how exact they have to be, the bound alone decides.
No kernel may reach another device: no remote copies, remote signals or barrier semaphores. Data moves between devices by JAX's collectives and lax.ppermute only.
A program may use at most 128 MiB of HBM per device.

```python
import jax
import jax.numpy as jnp

BLOCKS = 8192
VPB = 120
E_DEV = 4096
PROP_COL = 16
SENDERS = 32
ROWS_TILE = 2048
COLS_TILE = 1024
CAP = 576
VERTICES = 983040
EDGE_TILES = 1024
PROPOSALS = 128


def vertex_order(key):
    return jax.random.permutation(jax.random.fold_in(key, 11), VERTICES).astype(jnp.int32)


def draw_counts(key, part):
    count_key = jax.random.fold_in(key, 31)
    first_key, second_key = jax.random.split(count_key)
    upper_level = 9
    activity = jax.random.randint(first_key, (BLOCKS,), 1, upper_level, dtype=jnp.int32)
    widths = activity[:, None] * activity[None, :]
    upper = jax.random.randint(second_key, (BLOCKS, BLOCKS), 0, 1 + widths, dtype=jnp.int32)
    diagonal = 2 * jnp.eye(BLOCKS, dtype=jnp.int32)
    return (upper + upper.T + diagonal).astype(jnp.float32)


def draw_labels(key, part):
    order = vertex_order(key)
    inverse = jnp.argsort(order, stable=True).astype(jnp.int32)
    return (inverse % BLOCKS).astype(jnp.int32)


def draw_edge_tiles(key, part):
    order = vertex_order(key)
    edge_key = jax.random.fold_in(key, 23)
    row_tiles = BLOCKS // ROWS_TILE
    col_tiles = BLOCKS // COLS_TILE
    tile_count = row_tiles * col_tiles
    per_tile = CAP // 3
    slot_count = tile_count * per_tile
    hot_row = jax.random.randint(jax.random.fold_in(edge_key, 1), (), 0, row_tiles, dtype=jnp.int32)
    hot_col = (2 * hot_row + 2 + jax.random.randint(jax.random.fold_in(edge_key, 2), (), 0, col_tiles - 2, dtype=jnp.int32)) % col_tiles
    hot_tile = hot_row * col_tiles + hot_col
    first_pre = hot_col // 2 * col_tiles + 2 * hot_row
    second_pre = first_pre + 1
    half_bit = hot_col % 2
    offsets = jax.random.randint(jax.random.fold_in(edge_key, 3), (tile_count,), 0, 65536, dtype=jnp.int32)
    device_keys = jax.random.split(jax.random.fold_in(edge_key, 4), SENDERS)

    def one_device(device_key):
        keys = jax.random.split(device_key, 7)
        slots = jnp.arange(slot_count, dtype=jnp.int32)
        slot_tile = slots // per_tile
        noise = jax.random.randint(keys[0], (slot_count,), 0, 65536, dtype=jnp.int32)
        score = (noise + offsets[slot_tile]) * slot_count + slots
        forced = (slot_tile == hot_tile) | (slot_tile == first_pre) | (slot_tile == second_pre)
        score = jnp.where(forced, score - 2 ** 30, score)
        chosen = jnp.argsort(score, stable=True)[:E_DEV]
        tiles = slot_tile[chosen]
        tile_row = tiles // col_tiles
        tile_col = tiles % col_tiles
        pre_tile = (tiles == first_pre) | (tiles == second_pre)
        free_row = tile_row * ROWS_TILE + jax.random.randint(keys[1], (E_DEV,), 0, ROWS_TILE, dtype=jnp.int32)
        bound_row = tile_row * ROWS_TILE + half_bit * COLS_TILE + jax.random.randint(keys[2], (E_DEV,), 0, COLS_TILE, dtype=jnp.int32)
        row_block = jnp.where(pre_tile, bound_row, free_row)
        col_block = tile_col * COLS_TILE + jax.random.randint(keys[3], (E_DEV,), 0, COLS_TILE, dtype=jnp.int32)
        first_member = jax.random.randint(keys[4], (E_DEV,), 0, VPB, dtype=jnp.int32)
        second_member = jax.random.randint(keys[5], (E_DEV,), 0, VPB, dtype=jnp.int32)
        first_vertex = order[row_block + BLOCKS * first_member]
        second_vertex = order[col_block + BLOCKS * second_member]
        shuffle = jax.random.permutation(keys[6], E_DEV)
        first_vertex = first_vertex[shuffle].reshape(E_DEV // 128, 128)
        second_vertex = second_vertex[shuffle].reshape(E_DEV // 128, 128)
        return jnp.stack([first_vertex, second_vertex], axis=1)
    stacked = jax.vmap(one_device)(device_keys)
    return stacked.reshape(EDGE_TILES, 2, 128).astype(jnp.int32)


def draw_proposals(key, part):
    proposal_key = jax.random.fold_in(key, 41)
    groups = PROPOSALS // PROP_COL
    group_keys = jax.random.split(proposal_key, groups)

    def one_group(group_key, group_index):
        first_key, second_key = jax.random.split(group_key)
        picks = jax.random.permutation(first_key, COLS_TILE)[:PROP_COL].astype(jnp.int32)
        source = group_index * COLS_TILE + picks
        target = (source + 1 + jax.random.randint(second_key, (PROP_COL,), 0, BLOCKS - 1, dtype=jnp.int32)) % BLOCKS
        return (source, target)
    sources, targets = jax.vmap(one_group)(group_keys, jnp.arange(groups, dtype=jnp.int32))
    return jnp.stack([sources.reshape(-1), targets.reshape(-1)]).astype(jnp.int32)


def touch_ends(entries, key, least, largest):
    dims = entries.shape
    index_at = [jax.random.randint(jax.random.fold_in(key, axis), (), 0, dims[axis]) for axis in range(len(dims))]
    entries = entries.at[tuple(index_at)].set(least)
    longest = dims.index(max(dims))
    index_at[longest] = (index_at[longest] + 1) % dims[longest]
    return entries.at[tuple(index_at)].set(largest)


def setup_inputs(seed: int = 0) -> dict:
    key_list = jax.random.split(jax.random.key(seed), 6)
    return {
        "counts": draw_counts(jax.random.fold_in(key_list[5], 71), 0),
        "labels": draw_labels(jax.random.fold_in(key_list[5], 71), 0),
        "edge_tiles": draw_edge_tiles(jax.random.fold_in(key_list[5], 71), 0),
        "proposals": draw_proposals(jax.random.fold_in(key_list[5], 71), 0),
        "accept_flags": touch_ends((jax.random.randint(key_list[4], (PROPOSALS,), 0, 2) < 1).astype(jnp.int32), jax.random.fold_in(key_list[4], 1), 0, 1),
    }


def entropy_term(value):
    return value * jnp.log(jnp.maximum(value, 1.0))


def reference(counts, labels, edge_tiles, proposals, accept_flags):
    first_label = labels[edge_tiles[:, 0, :].reshape(-1)]
    second_label = labels[edge_tiles[:, 1, :].reshape(-1)]
    increments = jnp.zeros((BLOCKS, BLOCKS), jnp.float32).at[first_label, second_label].add(jnp.float32(1.0))
    count_matrix = counts + increments + increments.T
    source = proposals[0]
    target = proposals[1]
    own_row = count_matrix[source]
    other_row = count_matrix[target]
    positions = jnp.arange(BLOCKS, dtype=jnp.int32)
    at_source = positions[None, :] == source[:, None]
    at_target = positions[None, :] == target[:, None]
    mixed = entropy_term(own_row + other_row) - entropy_term(own_row) - entropy_term(other_row)
    pair_sum = jnp.sum(jnp.where(at_source | at_target, jnp.float32(0.0), mixed), axis=1)
    self_source = jnp.sum(jnp.where(at_source, own_row, jnp.float32(0.0)), axis=1)
    cross_count = jnp.sum(jnp.where(at_source, other_row, jnp.float32(0.0)), axis=1)
    self_target = jnp.sum(jnp.where(at_target, other_row, jnp.float32(0.0)), axis=1)
    degree_source = jnp.sum(own_row, axis=1)
    degree_target = jnp.sum(other_row, axis=1)
    corner = entropy_term(self_source + 2.0 * cross_count + self_target) - entropy_term(self_source) - entropy_term(self_target) - 2.0 * entropy_term(cross_count)
    change = -(pair_sum + 0.5 * corner) + entropy_term(degree_source + degree_target) - entropy_term(degree_source) - entropy_term(degree_target)
    merge_cost = change / BLOCKS
    accepted_cost = jnp.where(accept_flags == 1, merge_cost, jnp.float32(0.0))
    return count_matrix, merge_cost, accepted_cost
```

```python
import functools

import jax
import jax.numpy as jnp
from jax import lax
from jax.experimental import pallas as pl
from jax.experimental.pallas import tpu as pltpu
from jax.sharding import PartitionSpec as P

COPIES = 4


def entropy_term(value):
    return value * jnp.log(jnp.maximum(value, 1.0))


def log2_of(size):
    assert size & (size - 1) == 0
    return size.bit_length() - 1


def ingest_kernel(
    rows_shift, cols_shift, col_shift, devices, ids_smem, ids_ref, table_ref, out_ref, picked, labs, placed
):
    blocks = ids_ref.shape[0]
    slots = placed.shape[0]
    rows_mask = (1 << rows_shift) - 1
    cols_mask = (1 << cols_shift) - 1

    @pl.loop(0, blocks)
    def _(block):
        for lane in range(128):
            line = lax.shift_right_logical(ids_smem[block, lane], 7)
            picked[pl.ds(block * 128 + lane, 1), :] = table_ref[pl.ds(line, 1), :]

    sublane = lax.broadcasted_iota(jnp.int32, (128, 128), 0)

    @pl.loop(0, blocks // 4)
    def _(four):
        for step in range(4):
            block = four * 4 + step
            lines = picked[pl.ds(pl.multiple_of(block * 128, 128), 128), :].T
            lane = ids_ref[pl.ds(block, 1), :] & 127
            labs[pl.ds(block, 1), :] = jnp.sum(
                jnp.where(sublane == lane, lines, 0), axis=0, keepdims=True
            )

    placed[...] = jnp.zeros_like(placed)
    depth = lax.broadcasted_iota(jnp.int32, (128, 256), 0)
    width = lax.broadcasted_iota(jnp.int32, (128, 256), 1)
    upto = jnp.where((depth <= width) | (width >= 128), 1.0, 0.0).astype(jnp.bfloat16)
    owner_ids = lax.broadcasted_iota(jnp.int32, (devices, 128), 0)
    slot_ids = lax.broadcasted_iota(jnp.int32, (slots, 128), 0)
    group = 8

    def place(index, carry):
        row = labs[pl.ds(pl.multiple_of(index * group, group), group), :]
        col = jnp.concatenate([row[k ^ 1 : (k ^ 1) + 1, :] for k in range(group)], axis=0)
        owner = ((row >> rows_shift) << col_shift) + (col >> cols_shift)
        hot = [owner_ids == owner[k : k + 1, :] for k in range(group)]
        counted = jnp.dot(
            jnp.concatenate([jnp.where(h, 1.0, 0.0).astype(jnp.bfloat16) for h in hot], axis=0),
            upto,
            preferred_element_type=jnp.float32,
        )
        row_value = (row & rows_mask) + 1
        col_value = (col & cols_mask) + 1
        digits = [
            digit.astype(jnp.float32)
            for digit in (row_value >> 6, row_value & 63, col_value >> 6, col_value & 63)
        ]
        slot_parts = []
        digit_parts = []
        for k in range(group):
            part = counted[k * devices : (k + 1) * devices, :]
            rank = jnp.sum(jnp.where(hot[k], part[:, :128] + carry, 0.0), axis=0, keepdims=True)
            carry = carry + part[:, 128:]
            slot_parts.append(
                jnp.where(slot_ids == rank.astype(jnp.int32) - 1, 1.0, 0.0).astype(jnp.bfloat16)
            )
            digit_parts.append(
                jnp.concatenate(
                    [jnp.where(hot[k], d[k : k + 1, :], 0.0).astype(jnp.bfloat16) for d in digits],
                    axis=0,
                )
            )
        placed[...] += lax.dot_general(
            jnp.concatenate(slot_parts, axis=1),
            jnp.concatenate(digit_parts, axis=1),
            (((1,), (1,)), ((), ())),
            preferred_element_type=jnp.float32,
        )
        return carry

    lax.fori_loop(0, blocks // group, place, jnp.zeros((devices, 128), jnp.float32))
    flat = placed[...].T.astype(jnp.int32)
    out_ref[:, 0, :] = flat[:devices] * 64 + flat[devices : 2 * devices] - 1
    out_ref[:, 1, :] = flat[2 * devices : 3 * devices] * 64 + flat[3 * devices :] - 1


def ingest(labels, edge_tiles, rows_tile, cols_tile, col_devices, devices, slots):
    ids = edge_tiles.reshape(-1, 128)
    blocks = ids.shape[0]
    return pl.pallas_call(
        functools.partial(
            ingest_kernel, log2_of(rows_tile), log2_of(cols_tile), log2_of(col_devices), devices
        ),
        out_shape=jax.ShapeDtypeStruct((devices, 2, slots), jnp.int32),
        in_specs=[
            pl.BlockSpec(memory_space=pltpu.SMEM),
            pl.BlockSpec(memory_space=pltpu.VMEM),
            pl.BlockSpec(memory_space=pltpu.VMEM),
        ],
        out_specs=pl.BlockSpec(memory_space=pltpu.VMEM),
        scratch_shapes=[
            pltpu.VMEM((blocks * 128, 128), jnp.int32),
            pltpu.VMEM((blocks, 128), jnp.int32),
            pltpu.VMEM((slots, 4 * devices), jnp.float32),
        ],
        name="ingest",
    )(ids, ids, labels.reshape(-1, 128))


def scatter_kernel(
    capacity, cols_tiles, words, proposals, counts, out, source_rows, target_rows, copies, main, sem_in, sem_out
):
    total = counts.shape[0]
    arrive = pltpu.make_async_copy(counts, main.at[pl.ds(0, total)], sem_in)
    arrive.start()
    zeros = jnp.zeros((128, 128), jnp.float32)
    for copy in copies:

        @pl.loop(0, total // 128)
        def _(i):
            copy[pl.ds(pl.multiple_of(i * 128, 128), 128), :] = zeros

    arrive.wait()
    lanes = lax.broadcasted_iota(jnp.int32, (1, 128), 1)
    sums = (main,) + tuple(copies)

    @pl.loop(0, words.shape[0])
    def _(sender):
        for slot in range(capacity):
            word = words[sender, slot]
            line = pl.ds(lax.shift_right_logical(word, 7), 1)
            hot = (jnp.full((1, 128), word, jnp.int32) & 127) == lanes
            sums[slot % len(sums)][line, :] += jnp.where(hot, 1.0, 0.0)

    chunk = total // 8
    for n in range(8):

        @pl.loop(0, chunk // 64)
        def _(i):
            at = pl.ds(pl.multiple_of(n * chunk + i * 64, 64), 64)
            value = main[at, :]
            for copy in copies:
                value = value + copy[at, :]
            main[at, :] = value

        at = pl.ds(n * chunk, chunk)
        pltpu.make_async_copy(main.at[at], out.at[at], sem_out).start()

    rows_tile = total // cols_tiles
    first = lax.axis_index("row") * rows_tile
    mine = source_rows.shape[0]
    offset = lax.axis_index("row") * mine

    def line_of(row):
        return pl.ds(((row >> 3) * cols_tiles << 3) + (row & 7), cols_tiles, stride=8)

    @pl.loop(0, mine)
    def _(p):
        source_rows[p] = main[line_of(proposals[0, offset + p] - first), :]

    @pl.loop(0, target_rows.shape[0])
    def _(p):
        row = proposals[1, p] - first
        here = (row >= 0) & (row < rows_tile)
        value = main[line_of(jnp.where(here, row, 0)), :]
        target_rows[p] = value * jnp.where(here, 1.0, 0.0)

    pltpu.make_async_copy(main.at[pl.ds(0, total)], out, sem_out).wait()


def scatter(counts, words, proposals, capacity, row_devices):
    rows_tile, cols_tile = counts.shape
    cols_tiles = cols_tile // 128
    lines = counts.reshape(rows_tile // 8, 8, cols_tiles, 128).transpose(0, 2, 1, 3).reshape(-1, 128)
    total = lines.shape[0]
    count = proposals.shape[1]
    out, source_rows, target_rows = pl.pallas_call(
        functools.partial(scatter_kernel, capacity, cols_tiles),
        out_shape=(
            jax.ShapeDtypeStruct(lines.shape, jnp.float32),
            jax.ShapeDtypeStruct((count // row_devices, cols_tiles, 128), jnp.float32),
            jax.ShapeDtypeStruct((count, cols_tiles, 128), jnp.float32),
        ),
        in_specs=[
            pl.BlockSpec(memory_space=pltpu.SMEM),
            pl.BlockSpec(memory_space=pltpu.SMEM),
            pl.BlockSpec(memory_space=pl.ANY),
        ],
        out_specs=(
            pl.BlockSpec(memory_space=pl.ANY),
            pl.BlockSpec(memory_space=pltpu.VMEM),
            pl.BlockSpec(memory_space=pltpu.VMEM),
        ),
        scratch_shapes=[
            tuple(pltpu.VMEM((total + 8, 128), jnp.float32) for _ in range(COPIES - 1)),
            pltpu.VMEM((total + 8, 128), jnp.float32),
            pltpu.SemaphoreType.DMA,
            pltpu.SemaphoreType.DMA,
        ],
        compiler_params=pltpu.CompilerParams(vmem_limit_bytes=60000000),
        name="scatter",
    )(words, proposals, lines)
    updated = out.reshape(rows_tile // 8, cols_tiles, 8, 128).transpose(0, 2, 1, 3).reshape(rows_tile, cols_tile)
    return updated, source_rows, target_rows


def per_device(counts, labels, edge_tiles, proposals, accept_flags):
    rows_tile, cols_tile = counts.shape
    row_devices = lax.axis_size("row")
    col_devices = lax.axis_size("col")
    devices = row_devices * col_devices
    edge_count = edge_tiles.shape[0] * edge_tiles.shape[2]
    capacity = 9 * edge_count // (2 * devices)
    slots = -(-capacity // 128) * 128
    outgoing = ingest(labels, edge_tiles, rows_tile, cols_tile, col_devices, devices, slots)
    arrived = lax.all_to_all(outgoing, ("row", "col"), split_axis=0, concat_axis=0, tiled=True)
    row, col = arrived[:, 0, :], arrived[:, 1, :]
    line = (((row >> 3) * (cols_tile // 128) + (col >> 7)) << 3) + (row & 7)
    words = jnp.where(row >= 0, (line << 7) + (col & 127), rows_tile * cols_tile)
    updated, own, targets = scatter(counts, words, proposals, capacity, row_devices)

    proposal_count = proposals.shape[1]
    mine = proposal_count // row_devices
    row_index = lax.axis_index("row")
    col_index = lax.axis_index("col")
    other = jnp.sum(
        lax.all_to_all(
            targets.reshape((row_devices, mine) + targets.shape[1:]), "row", split_axis=0, concat_axis=0, tiled=True
        ),
        axis=0,
    )
    pairs = lax.dynamic_slice_in_dim(proposals, row_index * mine, mine, 1)
    position = (
        col_index * cols_tile
        + 128 * lax.broadcasted_iota(jnp.int32, own.shape, 1)
        + lax.broadcasted_iota(jnp.int32, own.shape, 2)
    )
    at_source = position == pairs[0][:, None, None]
    at_target = position == pairs[1][:, None, None]
    mixed = entropy_term(own + other) - entropy_term(own) - entropy_term(other)
    zero = jnp.float32(0.0)
    parts = jnp.stack(
        [
            jnp.sum(jnp.where(at_source | at_target, zero, mixed), axis=(1, 2)),
            jnp.sum(jnp.where(at_source, own, zero), axis=(1, 2)),
            jnp.sum(jnp.where(at_source, other, zero), axis=(1, 2)),
            jnp.sum(jnp.where(at_target, other, zero), axis=(1, 2)),
            jnp.sum(own, axis=(1, 2)),
            jnp.sum(other, axis=(1, 2)),
        ]
    )
    spread = lax.dynamic_update_slice(
        jnp.zeros((parts.shape[0], proposal_count), jnp.float32), parts, (0, row_index * mine)
    )
    per_col = accept_flags.shape[0]
    sums = lax.dynamic_slice_in_dim(lax.psum(spread, ("row", "col")), col_index * per_col, per_col, 1)
    pair_sum, self_source, cross_count, self_target, degree_source, degree_target = sums
    corner = (
        entropy_term(self_source + 2.0 * cross_count + self_target)
        - entropy_term(self_source)
        - entropy_term(self_target)
        - 2.0 * entropy_term(cross_count)
    )
    change = (
        -(pair_sum + 0.5 * corner)
        + entropy_term(degree_source + degree_target)
        - entropy_term(degree_source)
        - entropy_term(degree_target)
    )
    merge_cost = change / (rows_tile * row_devices)
    accepted_cost = jnp.where(accept_flags == 1, merge_cost, zero)
    return (updated, merge_cost, accepted_cost)


def solution(mesh):
    return jax.shard_map(
        per_device,
        mesh=mesh,
        in_specs=(P("row", "col"), P(), P(("row", "col"), None, None), P(), P("col")),
        out_specs=(P("row", "col"), P("col"), P("col")),
        check_vma=False,
    )
```

```python
import functools

import jax
import jax.numpy as jnp
from jax import lax
from jax.experimental import pallas as pl
from jax.experimental.pallas import tpu as pltpu
from jax.sharding import PartitionSpec as P

COPIES = 4


def entropy_term(value):
    return value * jnp.log(jnp.maximum(value, 1.0))


def log2_of(size):
    assert size & (size - 1) == 0
    return size.bit_length() - 1


def ingest_kernel(
    rows_shift, cols_shift, col_shift, devices, ids_smem, ids_ref, table_ref, out_ref, picked, labs, placed
):
    blocks = ids_ref.shape[0]
    slots = placed.shape[0]
    rows_mask = (1 << rows_shift) - 1
    cols_mask = (1 << cols_shift) - 1

    @pl.loop(0, blocks)
    def _(block):
        for lane in range(128):
            line = lax.shift_right_logical(ids_smem[block, lane], 7)
            picked[pl.ds(block * 128 + lane, 1), :] = table_ref[pl.ds(line, 1), :]

    sublane = lax.broadcasted_iota(jnp.int32, (128, 128), 0)

    @pl.loop(0, blocks // 4)
    def _(four):
        for step in range(4):
            block = four * 4 + step
            lines = picked[pl.ds(pl.multiple_of(block * 128, 128), 128), :].T
            lane = ids_ref[pl.ds(block, 1), :] & 127
            labs[pl.ds(block, 1), :] = jnp.sum(
                jnp.where(sublane == lane, lines, 0), axis=0, keepdims=True
            )

    placed[...] = jnp.zeros_like(placed)
    depth = lax.broadcasted_iota(jnp.int32, (128, 256), 0)
    width = lax.broadcasted_iota(jnp.int32, (128, 256), 1)
    upto = jnp.where((depth <= width) | (width >= 128), 1.0, 0.0).astype(jnp.bfloat16)
    owner_ids = lax.broadcasted_iota(jnp.int32, (devices, 128), 0)
    slot_ids = lax.broadcasted_iota(jnp.int32, (slots, 128), 0)
    group = 8

    def place(index, carry):
        row = labs[pl.ds(pl.multiple_of(index * group, group), group), :]
        col = jnp.concatenate([row[k ^ 1 : (k ^ 1) + 1, :] for k in range(group)], axis=0)
        owner = ((row >> rows_shift) << col_shift) + (col >> cols_shift)
        hot = [owner_ids == owner[k : k + 1, :] for k in range(group)]
        counted = jnp.dot(
            jnp.concatenate([jnp.where(h, 1.0, 0.0).astype(jnp.bfloat16) for h in hot], axis=0),
            upto,
            preferred_element_type=jnp.float32,
        )
        row_value = (row & rows_mask) + 1
        col_value = (col & cols_mask) + 1
        digits = [
            digit.astype(jnp.float32)
            for digit in (row_value >> 6, row_value & 63, col_value >> 6, col_value & 63)
        ]
        slot_parts = []
        digit_parts = []
        for k in range(group):
            part = counted[k * devices : (k + 1) * devices, :]
            rank = jnp.sum(jnp.where(hot[k], part[:, :128] + carry, 0.0), axis=0, keepdims=True)
            carry = carry + part[:, 128:]
            slot_parts.append(
                jnp.where(slot_ids == rank.astype(jnp.int32) - 1, 1.0, 0.0).astype(jnp.bfloat16)
            )
            digit_parts.append(
                jnp.concatenate(
                    [jnp.where(hot[k], d[k : k + 1, :], 0.0).astype(jnp.bfloat16) for d in digits],
                    axis=0,
                )
            )
        placed[...] += lax.dot_general(
            jnp.concatenate(slot_parts, axis=1),
            jnp.concatenate(digit_parts, axis=1),
            (((1,), (1,)), ((), ())),
            preferred_element_type=jnp.float32,
        )
        return carry

    lax.fori_loop(0, blocks // group, place, jnp.zeros((devices, 128), jnp.float32))
    flat = placed[...].T.astype(jnp.int32)
    out_ref[:, 0, :] = flat[:devices] * 64 + flat[devices : 2 * devices] - 1
    out_ref[:, 1, :] = flat[2 * devices : 3 * devices] * 64 + flat[3 * devices :] - 1


def ingest(labels, edge_tiles, rows_tile, cols_tile, col_devices, devices, slots):
    ids = edge_tiles.reshape(-1, 128)
    blocks = ids.shape[0]
    return pl.pallas_call(
        functools.partial(
            ingest_kernel, log2_of(rows_tile), log2_of(cols_tile), log2_of(col_devices), devices
        ),
        out_shape=jax.ShapeDtypeStruct((devices, 2, slots), jnp.int32),
        in_specs=[
            pl.BlockSpec(memory_space=pltpu.SMEM),
            pl.BlockSpec(memory_space=pltpu.VMEM),
            pl.BlockSpec(memory_space=pltpu.VMEM),
        ],
        out_specs=pl.BlockSpec(memory_space=pltpu.VMEM),
        scratch_shapes=[
            pltpu.VMEM((blocks * 128, 128), jnp.int32),
            pltpu.VMEM((blocks, 128), jnp.int32),
            pltpu.VMEM((slots, 4 * devices), jnp.float32),
        ],
        name="ingest",
    )(ids, ids, labels.reshape(-1, 128))


def scatter_kernel(
    capacity, cols_tiles, words, proposals, counts, out, source_rows, target_rows, copies, main, sem_in, sem_out
):
    total = counts.shape[0]
    arrive = pltpu.make_async_copy(counts, main.at[pl.ds(0, total)], sem_in)
    arrive.start()
    zeros = jnp.zeros((128, 128), jnp.float32)
    for copy in copies:

        @pl.loop(0, total // 128)
        def _(i):
            copy[pl.ds(pl.multiple_of(i * 128, 128), 128), :] = zeros

    arrive.wait()
    lanes = lax.broadcasted_iota(jnp.int32, (1, 128), 1)
    sums = (main,) + tuple(copies)

    @pl.loop(0, words.shape[0])
    def _(sender):
        for slot in range(capacity):
            word = words[sender, slot]
            line = pl.ds(lax.shift_right_logical(word, 7), 1)
            hot = (jnp.full((1, 128), word, jnp.int32) & 127) == lanes
            sums[slot % len(sums)][line, :] += jnp.where(hot, 1.0, 0.0)

    chunk = total // 8
    for n in range(8):

        @pl.loop(0, chunk // 64)
        def _(i):
            at = pl.ds(pl.multiple_of(n * chunk + i * 64, 64), 64)
            value = main[at, :]
            for copy in copies:
                value = value + copy[at, :]
            main[at, :] = value

        at = pl.ds(n * chunk, chunk)
        pltpu.make_async_copy(main.at[at], out.at[at], sem_out).start()

    rows_tile = total // cols_tiles
    first = lax.axis_index("row") * rows_tile
    mine = source_rows.shape[0]
    offset = lax.axis_index("row") * mine

    def line_of(row):
        return pl.ds(((row >> 3) * cols_tiles << 3) + (row & 7), cols_tiles, stride=8)

    @pl.loop(0, mine)
    def _(p):
        source_rows[p] = main[line_of(proposals[0, offset + p] - first), :]

    @pl.loop(0, target_rows.shape[0])
    def _(p):
        row = proposals[1, p] - first
        here = (row >= 0) & (row < rows_tile)
        value = main[line_of(jnp.where(here, row, 0)), :]
        target_rows[p] = value * jnp.where(here, 1.0, 0.0)

    pltpu.make_async_copy(main.at[pl.ds(0, total)], out, sem_out).wait()


def scatter(counts, words, proposals, capacity, row_devices):
    rows_tile, cols_tile = counts.shape
    cols_tiles = cols_tile // 128
    lines = counts.reshape(rows_tile // 8, 8, cols_tiles, 128).transpose(0, 2, 1, 3).reshape(-1, 128)
    total = lines.shape[0]
    count = proposals.shape[1]
    out, source_rows, target_rows = pl.pallas_call(
        functools.partial(scatter_kernel, capacity, cols_tiles),
        out_shape=(
            jax.ShapeDtypeStruct(lines.shape, jnp.float32),
            jax.ShapeDtypeStruct((count // row_devices, cols_tiles, 128), jnp.float32),
            jax.ShapeDtypeStruct((count, cols_tiles, 128), jnp.float32),
        ),
        in_specs=[
            pl.BlockSpec(memory_space=pltpu.SMEM),
            pl.BlockSpec(memory_space=pltpu.SMEM),
            pl.BlockSpec(memory_space=pl.ANY),
        ],
        out_specs=(
            pl.BlockSpec(memory_space=pl.ANY),
            pl.BlockSpec(memory_space=pltpu.VMEM),
            pl.BlockSpec(memory_space=pltpu.VMEM),
        ),
        scratch_shapes=[
            tuple(pltpu.VMEM((total + 8, 128), jnp.float32) for _ in range(COPIES - 1)),
            pltpu.VMEM((total + 8, 128), jnp.float32),
            pltpu.SemaphoreType.DMA,
            pltpu.SemaphoreType.DMA,
        ],
        compiler_params=pltpu.CompilerParams(vmem_limit_bytes=60000000),
        name="scatter",
    )(words, proposals, lines)
    updated = out.reshape(rows_tile // 8, cols_tiles, 8, 128).transpose(0, 2, 1, 3).reshape(rows_tile, cols_tile)
    return updated, source_rows, target_rows


def per_device(counts, labels, edge_tiles, proposals, accept_flags):
    rows_tile, cols_tile = counts.shape
    row_devices = lax.axis_size("row")
    col_devices = lax.axis_size("col")
    devices = row_devices * col_devices
    edge_count = edge_tiles.shape[0] * edge_tiles.shape[2]
    capacity = 9 * edge_count // (2 * devices)
    slots = -(-capacity // 128) * 128
    outgoing = ingest(labels, edge_tiles, rows_tile, cols_tile, col_devices, devices, slots)
    arrived = lax.all_to_all(outgoing, ("row", "col"), split_axis=0, concat_axis=0, tiled=True)
    row, col = arrived[:, 0, :], arrived[:, 1, :]
    line = (((row >> 3) * (cols_tile // 128) + (col >> 7)) << 3) + (row & 7)
    words = jnp.where(row >= 0, (line << 7) + (col & 127), rows_tile * cols_tile)
    updated, own, targets = scatter(counts, words, proposals, capacity, row_devices)

    proposal_count = proposals.shape[1]
    mine = proposal_count // row_devices
    row_index = lax.axis_index("row")
    col_index = lax.axis_index("col")
    other = targets.reshape((row_devices, mine) + targets.shape[1:])
    for bit in range(log2_of(row_devices)):
        halves = other.reshape((-1, 2) + other.shape[1:])
        side = (row_index >> bit) & 1
        swapped = lax.ppermute(
            lax.dynamic_index_in_dim(halves, 1 - side, 1, keepdims=False),
            "row",
            [(device, device ^ (1 << bit)) for device in range(row_devices)],
        )
        other = lax.dynamic_index_in_dim(halves, side, 1, keepdims=False) + swapped
    other = other[0]
    pairs = lax.dynamic_slice_in_dim(proposals, row_index * mine, mine, 1)
    position = (
        col_index * cols_tile
        + 128 * lax.broadcasted_iota(jnp.int32, own.shape, 1)
        + lax.broadcasted_iota(jnp.int32, own.shape, 2)
    )
    at_source = position == pairs[0][:, None, None]
    at_target = position == pairs[1][:, None, None]
    mixed = entropy_term(own + other) - entropy_term(own) - entropy_term(other)
    zero = jnp.float32(0.0)
    parts = jnp.stack(
        [
            jnp.sum(jnp.where(at_source | at_target, zero, mixed), axis=(1, 2)),
            jnp.sum(jnp.where(at_source, own, zero), axis=(1, 2)),
            jnp.sum(jnp.where(at_source, other, zero), axis=(1, 2)),
            jnp.sum(jnp.where(at_target, other, zero), axis=(1, 2)),
            jnp.sum(own, axis=(1, 2)),
            jnp.sum(other, axis=(1, 2)),
        ]
    )
    per_col = accept_flags.shape[0]
    width = -(-parts.shape[0] * per_col // 128) * 128
    groups = mine // per_col
    lines = parts.reshape(-1, groups, per_col).transpose(1, 0, 2).reshape(groups, -1)
    lines = jnp.pad(lines, ((0, 0), (0, width - lines.shape[1])))
    spread = jnp.where(
        jnp.arange(row_devices)[:, None, None] == row_index, lines[None], zero
    ).reshape(1, col_devices, 1, width)
    spread = jnp.broadcast_to(spread, (row_devices, col_devices, 1, width)).reshape(devices, 1, width)
    gathered = lax.all_to_all(spread, ("row", "col"), split_axis=0, concat_axis=0, tiled=True)
    sums = jnp.sum(gathered, axis=(0, 1))[: parts.shape[0] * per_col].reshape(-1, per_col)
    pair_sum, self_source, cross_count, self_target, degree_source, degree_target = sums
    corner = (
        entropy_term(self_source + 2.0 * cross_count + self_target)
        - entropy_term(self_source)
        - entropy_term(self_target)
        - 2.0 * entropy_term(cross_count)
    )
    change = (
        -(pair_sum + 0.5 * corner)
        + entropy_term(degree_source + degree_target)
        - entropy_term(degree_source)
        - entropy_term(degree_target)
    )
    merge_cost = change / (rows_tile * row_devices)
    accepted_cost = jnp.where(accept_flags == 1, merge_cost, zero)
    return (updated, merge_cost, accepted_cost)


def solution(mesh):
    return jax.shard_map(
        per_device,
        mesh=mesh,
        in_specs=(P("row", "col"), P(), P(("row", "col"), None, None), P(), P("col")),
        out_specs=(P("row", "col"), P("col"), P("col")),
        check_vma=False,
    )
```

```python
import functools

import jax
import jax.numpy as jnp
from jax import lax
from jax.experimental import pallas as pl
from jax.experimental.pallas import tpu as pltpu
from jax.sharding import PartitionSpec as P

COPIES = 5
GROUP = 4


def entropy_term(value):
    return value * jnp.log(jnp.maximum(value, 1.0))


def log2_of(size):
    assert size & (size - 1) == 0
    return size.bit_length() - 1


def ingest_kernel(rows_shift, cols_shift, col_shift, devices, ids_smem, ids_ref, table_ref, out_ref, picked, placed):
    blocks = ids_ref.shape[0]
    slots = placed.shape[0]
    group = picked.shape[0] // 128
    rows_mask = (1 << rows_shift) - 1
    cols_mask = (1 << cols_shift) - 1

    def pick(index):
        for k in range(group):
            for lane in range(128):
                line = lax.shift_right_logical(ids_smem[index * group + k, lane], 7)
                picked[k * 128 + lane : k * 128 + lane + 1, :] = table_ref[pl.ds(line, 1), :]

    placed[...] = jnp.zeros_like(placed)
    sublane = lax.broadcasted_iota(jnp.int32, (128, 128), 0)
    depth = lax.broadcasted_iota(jnp.int32, (128, 256), 0)
    width = lax.broadcasted_iota(jnp.int32, (128, 256), 1)
    upto = jnp.where((depth <= width) | (width >= 128), 1.0, 0.0).astype(jnp.bfloat16)
    owner_ids = lax.broadcasted_iota(jnp.int32, (devices, 128), 0)
    slot_ids = lax.broadcasted_iota(jnp.int32, (slots, 128), 0)
    steps = blocks // group
    pick(0)

    def place(index, carry):
        turned = [picked[k * 128 : (k + 1) * 128, :].T for k in range(group)]
        pick(jnp.minimum(index + 1, steps - 1))
        label = [
            jnp.sum(
                jnp.where(sublane == (ids_ref[pl.ds(index * group + k, 1), :] & 127), turned[k], 0),
                axis=0,
                keepdims=True,
            )
            for k in range(group)
        ]
        row = jnp.concatenate(label, axis=0)
        col = jnp.concatenate([label[k ^ 1] for k in range(group)], axis=0)
        owner = ((row >> rows_shift) << col_shift) + (col >> cols_shift)
        hot = [owner_ids == owner[k : k + 1, :] for k in range(group)]
        counted = jnp.dot(
            jnp.concatenate([jnp.where(h, 1.0, 0.0).astype(jnp.bfloat16) for h in hot], axis=0),
            upto,
            preferred_element_type=jnp.float32,
        )
        row_value = (row & rows_mask) + 1
        col_value = (col & cols_mask) + 1
        digits = [
            digit.astype(jnp.float32)
            for digit in (row_value >> 6, row_value & 63, col_value >> 6, col_value & 63)
        ]
        slot_parts = []
        digit_parts = []
        for k in range(group):
            part = counted[k * devices : (k + 1) * devices, :]
            rank = jnp.sum(jnp.where(hot[k], part[:, :128] + carry, 0.0), axis=0, keepdims=True)
            carry = carry + part[:, 128:]
            slot_parts.append(
                jnp.where(slot_ids == rank.astype(jnp.int32) - 1, 1.0, 0.0).astype(jnp.bfloat16)
            )
            digit_parts.append(
                jnp.concatenate(
                    [jnp.where(hot[k], d[k : k + 1, :], 0.0).astype(jnp.bfloat16) for d in digits],
                    axis=0,
                )
            )
        placed[...] += lax.dot_general(
            jnp.concatenate(slot_parts, axis=1),
            jnp.concatenate(digit_parts, axis=1),
            (((1,), (1,)), ((), ())),
            preferred_element_type=jnp.float32,
        )
        return carry

    lax.fori_loop(0, steps, place, jnp.zeros((devices, 128), jnp.float32))
    flat = placed[...].T.astype(jnp.int32)
    out_ref[:, 0, :] = flat[:devices] * 64 + flat[devices : 2 * devices] - 1
    out_ref[:, 1, :] = flat[2 * devices : 3 * devices] * 64 + flat[3 * devices :] - 1


def ingest(labels, edge_tiles, rows_tile, cols_tile, col_devices, devices, slots):
    ids = edge_tiles.reshape(-1, 128)
    return pl.pallas_call(
        functools.partial(
            ingest_kernel, log2_of(rows_tile), log2_of(cols_tile), log2_of(col_devices), devices
        ),
        out_shape=jax.ShapeDtypeStruct((devices, 2, slots), jnp.int32),
        in_specs=[
            pl.BlockSpec(memory_space=pltpu.SMEM),
            pl.BlockSpec(memory_space=pltpu.VMEM),
            pl.BlockSpec(memory_space=pltpu.VMEM),
        ],
        out_specs=pl.BlockSpec(memory_space=pltpu.VMEM),
        scratch_shapes=[
            pltpu.VMEM((GROUP * 128, 128), jnp.int32),
            pltpu.VMEM((slots, 4 * devices), jnp.float32),
        ],
        name="ingest",
    )(ids, ids, labels.reshape(-1, 128))


def scatter_kernel(
    capacity,
    cols_tiles,
    words_hbm,
    proposals,
    counts,
    out,
    source_rows,
    target_rows,
    copies,
    main,
    words,
    sem_in,
    sem_words,
    sem_out,
):
    total = counts.shape[0]
    arrive = pltpu.make_async_copy(counts, main.at[pl.ds(0, total)], sem_in)
    arrive.start()
    listed = pltpu.make_async_copy(words_hbm, words, sem_words)
    listed.start()
    zeros = jnp.zeros((256, 128), jnp.float32)
    for copy in copies:

        @pl.loop(0, total // 256)
        def _(i):
            copy[pl.ds(pl.multiple_of(i * 256, 256), 256), :] = zeros

    listed.wait()
    arrive.wait()
    lanes = lax.broadcasted_iota(jnp.int32, (1, 128), 1)
    sums = (main,) + tuple(copies)

    def add_line(at, count):
        for slot in range(count):
            word = words[at, slot]
            line = pl.ds(lax.shift_right_logical(word, 7), 1)
            hot = (jnp.full((1, 128), word, jnp.int32) & 127) == lanes
            sums[slot % len(sums)][line, :] += jnp.where(hot, 1.0, 0.0)

    per_sender = -(-capacity // 128)
    whole, rest = capacity // 128, capacity % 128

    @pl.loop(0, words.shape[0] // per_sender)
    def _(sender):
        if whole:

            @pl.loop(0, whole)
            def _(part):
                add_line(sender * per_sender + part, 128)

        if rest:
            add_line(sender * per_sender + whole, rest)

    chunk = total // 8
    for n in range(8):

        @pl.loop(0, chunk // 64)
        def _(i):
            at = pl.ds(pl.multiple_of(n * chunk + i * 64, 64), 64)
            value = main[at, :]
            for copy in copies:
                value = value + copy[at, :]
            main[at, :] = value

        at = pl.ds(n * chunk, chunk)
        pltpu.make_async_copy(main.at[at], out.at[at], sem_out).start()

    rows_tile = total // cols_tiles
    first = lax.axis_index("row") * rows_tile
    mine = source_rows.shape[0]
    offset = lax.axis_index("row") * mine

    def line_of(row):
        return pl.ds(((row >> 3) * cols_tiles << 3) + (row & 7), cols_tiles, stride=8)

    @pl.loop(0, mine, unroll=8)
    def _(p):
        source_rows[p] = main[line_of(proposals[0, offset + p] - first), :]

    @pl.loop(0, target_rows.shape[0], unroll=8)
    def _(p):
        row = proposals[1, p] - first
        here = (row >= 0) & (row < rows_tile)
        value = main[line_of(jnp.where(here, row, 0)), :]
        target_rows[p] = value * jnp.where(here, 1.0, 0.0)

    pltpu.make_async_copy(main.at[pl.ds(0, total)], out, sem_out).wait()


def scatter(counts, words, proposals, capacity, row_devices):
    rows_tile, cols_tile = counts.shape
    cols_tiles = cols_tile // 128
    lines = counts.reshape(rows_tile // 8, 8, cols_tiles, 128).transpose(0, 2, 1, 3).reshape(-1, 128)
    total = lines.shape[0]
    count = proposals.shape[1]
    out, source_rows, target_rows = pl.pallas_call(
        functools.partial(scatter_kernel, capacity, cols_tiles),
        out_shape=(
            jax.ShapeDtypeStruct(lines.shape, jnp.float32),
            jax.ShapeDtypeStruct((count // row_devices, cols_tiles, 128), jnp.float32),
            jax.ShapeDtypeStruct((count, cols_tiles, 128), jnp.float32),
        ),
        in_specs=[
            pl.BlockSpec(memory_space=pl.ANY),
            pl.BlockSpec(memory_space=pltpu.SMEM),
            pl.BlockSpec(memory_space=pl.ANY),
        ],
        out_specs=(
            pl.BlockSpec(memory_space=pl.ANY),
            pl.BlockSpec(memory_space=pltpu.VMEM),
            pl.BlockSpec(memory_space=pltpu.VMEM),
        ),
        scratch_shapes=[
            tuple(pltpu.VMEM((total + 8, 128), jnp.float32) for _ in range(COPIES - 1)),
            pltpu.VMEM((total + 8, 128), jnp.float32),
            pltpu.SMEM(words.shape, jnp.int32),
            pltpu.SemaphoreType.DMA,
            pltpu.SemaphoreType.DMA,
            pltpu.SemaphoreType.DMA,
        ],
        compiler_params=pltpu.CompilerParams(vmem_limit_bytes=60000000),
        name="scatter",
    )(words, proposals, lines)
    updated = out.reshape(rows_tile // 8, cols_tiles, 8, 128).transpose(0, 2, 1, 3).reshape(rows_tile, cols_tile)
    return updated, source_rows, target_rows


def per_device(counts, labels, edge_tiles, proposals, accept_flags):
    rows_tile, cols_tile = counts.shape
    row_devices = lax.axis_size("row")
    col_devices = lax.axis_size("col")
    devices = row_devices * col_devices
    edge_count = edge_tiles.shape[0] * edge_tiles.shape[2]
    capacity = 9 * edge_count // (2 * devices)
    slots = -(-capacity // 128) * 128
    outgoing = ingest(labels, edge_tiles, rows_tile, cols_tile, col_devices, devices, slots)
    arrived = lax.all_to_all(outgoing, ("row", "col"), split_axis=0, concat_axis=0, tiled=True)
    row, col = arrived[:, 0, :], arrived[:, 1, :]
    line = (((row >> 3) * (cols_tile // 128) + (col >> 7)) << 3) + (row & 7)
    words = jnp.where(row >= 0, (line << 7) + (col & 127), rows_tile * cols_tile).reshape(-1, 128)
    updated, own, targets = scatter(counts, words, proposals, capacity, row_devices)

    proposal_count = proposals.shape[1]
    mine = proposal_count // row_devices
    row_index = lax.axis_index("row")
    col_index = lax.axis_index("col")
    other = targets.reshape((row_devices, mine) + targets.shape[1:])
    for bit in range(log2_of(row_devices)):
        halves = other.reshape((-1, 2) + other.shape[1:])
        side = (row_index >> bit) & 1
        swapped = lax.ppermute(
            lax.dynamic_index_in_dim(halves, 1 - side, 1, keepdims=False),
            "row",
            [(device, device ^ (1 << bit)) for device in range(row_devices)],
        )
        other = lax.dynamic_index_in_dim(halves, side, 1, keepdims=False) + swapped
    other = other[0]
    pairs = lax.dynamic_slice_in_dim(proposals, row_index * mine, mine, 1)
    position = (
        col_index * cols_tile
        + 128 * lax.broadcasted_iota(jnp.int32, own.shape, 1)
        + lax.broadcasted_iota(jnp.int32, own.shape, 2)
    )
    at_source = position == pairs[0][:, None, None]
    at_target = position == pairs[1][:, None, None]
    mixed = entropy_term(own + other) - entropy_term(own) - entropy_term(other)
    zero = jnp.float32(0.0)
    parts = jnp.stack(
        [
            jnp.sum(jnp.where(at_source | at_target, zero, mixed), axis=(1, 2)),
            jnp.sum(jnp.where(at_source, own, zero), axis=(1, 2)),
            jnp.sum(jnp.where(at_source, other, zero), axis=(1, 2)),
            jnp.sum(jnp.where(at_target, other, zero), axis=(1, 2)),
            jnp.sum(own, axis=(1, 2)),
            jnp.sum(other, axis=(1, 2)),
        ]
    )
    per_col = accept_flags.shape[0]
    width = -(-parts.shape[0] * per_col // 128) * 128
    groups = mine // per_col
    lines = parts.reshape(-1, groups, per_col).transpose(1, 0, 2).reshape(groups, -1)
    lines = jnp.pad(lines, ((0, 0), (0, width - lines.shape[1])))
    spread = jnp.where(
        jnp.arange(row_devices)[:, None, None] == row_index, lines[None], zero
    ).reshape(1, col_devices, 1, width)
    spread = jnp.broadcast_to(spread, (row_devices, col_devices, 1, width)).reshape(devices, 1, width)
    gathered = lax.all_to_all(spread, ("row", "col"), split_axis=0, concat_axis=0, tiled=True)
    sums = jnp.sum(gathered, axis=(0, 1))[: parts.shape[0] * per_col].reshape(-1, per_col)
    pair_sum, self_source, cross_count, self_target, degree_source, degree_target = sums
    corner = (
        entropy_term(self_source + 2.0 * cross_count + self_target)
        - entropy_term(self_source)
        - entropy_term(self_target)
        - 2.0 * entropy_term(cross_count)
    )
    change = (
        -(pair_sum + 0.5 * corner)
        + entropy_term(degree_source + degree_target)
        - entropy_term(degree_source)
        - entropy_term(degree_target)
    )
    merge_cost = change / (rows_tile * row_devices)
    accepted_cost = jnp.where(accept_flags == 1, merge_cost, zero)
    return (updated, merge_cost, accepted_cost)


def solution(mesh):
    return jax.shard_map(
        per_device,
        mesh=mesh,
        in_specs=(P("row", "col"), P(), P(("row", "col"), None, None), P(), P("col")),
        out_specs=(P("row", "col"), P("col"), P("col")),
        check_vma=False,
    )
```

```python
import functools

import jax
import jax.numpy as jnp
from jax import lax
from jax.experimental import pallas as pl
from jax.experimental.pallas import tpu as pltpu
from jax.sharding import PartitionSpec as P

COPIES = 5
GROUP = 8
SPARE = 32


def entropy_term(value):
    return value * jnp.log(jnp.maximum(value, 1.0))


def log2_of(size):
    assert size & (size - 1) == 0
    return size.bit_length() - 1


def ingest_kernel(
    rows_shift,
    cols_shift,
    col_shift,
    devices,
    ids_ref,
    table_hbm,
    out_ref,
    table_ref,
    lines_ref,
    lines_smem,
    picked,
    placed,
    sem_table,
    sem_lines,
):
    blocks = ids_ref.shape[0]
    slots = placed.shape[0]
    group = picked.shape[0] // 128
    rows_mask = (1 << rows_shift) - 1
    cols_mask = (1 << cols_shift) - 1

    def pick(index):
        for k in range(group):
            for lane in range(128):
                line = pl.ds(lines_smem[index * group + k, lane], 1)
                picked[k * 128 + lane : k * 128 + lane + 1, :] = table_ref[line, :]

    whole_table = pltpu.make_async_copy(table_hbm, table_ref, sem_table)
    whole_table.start()
    lines_ref[...] = ids_ref[...] >> 7
    lines = pltpu.make_async_copy(lines_ref, lines_smem, sem_lines)
    lines.start()
    placed[...] = jnp.zeros_like(placed)
    sublane = lax.broadcasted_iota(jnp.int32, (128, 128), 0)
    depth = lax.broadcasted_iota(jnp.int32, (128, 256), 0)
    width = lax.broadcasted_iota(jnp.int32, (128, 256), 1)
    upto = jnp.where((depth <= width) | (width >= 128), 1.0, 0.0).astype(jnp.bfloat16)
    owner_ids = lax.broadcasted_iota(jnp.int32, (devices, 128), 0)
    slot_ids = lax.broadcasted_iota(jnp.int32, (slots, 128), 0)
    steps = blocks // group
    lines.wait()
    whole_table.wait()
    pick(0)

    def place(index, carry, last=False):
        turned = [picked[k * 128 : (k + 1) * 128, :].T for k in range(group)]
        if not last:
            pick(index + 1)
        label = [
            jnp.sum(
                jnp.where(sublane == (ids_ref[pl.ds(index * group + k, 1), :] & 127), turned[k], 0),
                axis=0,
                keepdims=True,
            )
            for k in range(group)
        ]
        row = jnp.concatenate(label, axis=0)
        col = jnp.concatenate([label[k ^ 1] for k in range(group)], axis=0)
        owner = ((row >> rows_shift) << col_shift) + (col >> cols_shift)
        hot = [owner_ids == owner[k : k + 1, :] for k in range(group)]
        counted = jnp.dot(
            jnp.concatenate([jnp.where(h, 1.0, 0.0).astype(jnp.bfloat16) for h in hot], axis=0),
            upto,
            preferred_element_type=jnp.float32,
        )
        row_value = (row & rows_mask) + 1
        col_value = (col & cols_mask) + 1
        digits = [
            digit.astype(jnp.float32)
            for digit in (row_value >> 6, row_value & 63, col_value >> 6, col_value & 63)
        ]
        slot_parts = []
        digit_parts = []
        for k in range(group):
            part = counted[k * devices : (k + 1) * devices, :]
            rank = jnp.sum(jnp.where(hot[k], part[:, :128] + carry, 0.0), axis=0, keepdims=True)
            carry = carry + part[:, 128:]
            slot_parts.append(
                jnp.where(slot_ids == rank.astype(jnp.int32) - 1, 1.0, 0.0).astype(jnp.bfloat16)
            )
            digit_parts.append(
                jnp.concatenate(
                    [jnp.where(hot[k], d[k : k + 1, :], 0.0).astype(jnp.bfloat16) for d in digits],
                    axis=0,
                )
            )
        placed[...] += lax.dot_general(
            jnp.concatenate(slot_parts, axis=1),
            jnp.concatenate(digit_parts, axis=1),
            (((1,), (1,)), ((), ())),
            preferred_element_type=jnp.float32,
        )
        return carry

    place(steps - 1, lax.fori_loop(0, steps - 1, place, jnp.zeros((devices, 128), jnp.float32)), last=True)
    flat = placed[...].T.astype(jnp.int32)
    out_ref[:, 0, :] = flat[:devices] * 64 + flat[devices : 2 * devices] - 1
    out_ref[:, 1, :] = flat[2 * devices : 3 * devices] * 64 + flat[3 * devices :] - 1


def ingest(labels, edge_tiles, rows_tile, cols_tile, col_devices, devices, slots):
    ids = edge_tiles.reshape(-1, 128)
    table = labels.reshape(-1, 128)
    return pl.pallas_call(
        functools.partial(
            ingest_kernel, log2_of(rows_tile), log2_of(cols_tile), log2_of(col_devices), devices
        ),
        out_shape=jax.ShapeDtypeStruct((devices, 2, slots), jnp.int32),
        in_specs=[pl.BlockSpec(memory_space=pltpu.VMEM), pl.BlockSpec(memory_space=pl.ANY)],
        out_specs=pl.BlockSpec(memory_space=pltpu.VMEM),
        scratch_shapes=[
            pltpu.VMEM(table.shape, jnp.int32),
            pltpu.VMEM(ids.shape, jnp.int32),
            pltpu.SMEM(ids.shape, jnp.int32),
            pltpu.VMEM((GROUP * 128, 128), jnp.int32),
            pltpu.VMEM((slots, 4 * devices), jnp.float32),
            pltpu.SemaphoreType.DMA,
            pltpu.SemaphoreType.DMA,
        ],
        name="ingest",
    )(ids, table)


def scatter_kernel(
    capacity,
    arrived,
    proposals_hbm,
    counts,
    out,
    source_rows,
    kept_rows,
    sent_rows,
    copies,
    main,
    words_ref,
    words,
    proposals,
    source_ref,
    kept_ref,
    sent_ref,
    sem_counts,
    sem_words,
    sem_proposals,
    sem_rows,
    sem_out,
):
    total = counts.shape[0]
    senders = arrived.shape[0]
    parts = arrived.shape[2] // 128
    cols_tiles = source_ref.shape[1]
    arrive = pltpu.make_async_copy(counts, main.at[pl.ds(0, total)], sem_counts)
    arrive.start()
    asked = pltpu.make_async_copy(proposals_hbm, proposals, sem_proposals)
    asked.start()
    spare = total + (lax.broadcasted_iota(jnp.int32, (senders, 128), 1) & (SPARE - 1))
    spare = spare << 7
    for part in range(parts):
        row = arrived[:, 0, part * 128 : (part + 1) * 128]
        col = arrived[:, 1, part * 128 : (part + 1) * 128]
        line = (((row >> 3) * cols_tiles + (col >> 7)) << 3) + (row & 7)
        words_ref[pl.ds(part, senders, stride=parts), :] = jnp.where(
            row >= 0, (line << 7) + (col & 127), spare
        )
    listed = pltpu.make_async_copy(words_ref, words, sem_words)
    listed.start()
    zeros = jnp.zeros((256, 128), jnp.float32)
    for copy in copies:

        @pl.loop(0, total // 256)
        def _(i):
            copy[pl.ds(pl.multiple_of(i * 256, 256), 256), :] = zeros

    asked.wait()
    listed.wait()
    arrive.wait()
    lanes = lax.broadcasted_iota(jnp.int32, (1, 128), 1)
    sums = (main,) + tuple(copies)

    def add_line(at, count):
        for slot in range(count):
            word = words[at, slot]
            line = pl.ds(lax.shift_right_logical(word, 7), 1)
            hot = (jnp.full((1, 128), word, jnp.int32) & 127) == lanes
            sums[slot % len(sums)][line, :] += jnp.where(hot, 1.0, 0.0)

    whole, rest = capacity // 128, capacity % 128

    @pl.loop(0, senders)
    def _(sender):
        if whole:

            @pl.loop(0, whole)
            def _(part):
                add_line(sender * parts + part, 128)

        if rest:
            add_line(sender * parts + whole, rest)

    rows_tile = total // cols_tiles
    first = lax.axis_index("row") * rows_tile
    mine = source_ref.shape[0]
    offset = lax.axis_index("row") * mine

    def summed(row):
        at = pl.ds(((row >> 3) * cols_tiles << 3) + (row & 7), cols_tiles, stride=8)
        value = sums[0][at, :]
        for one in sums[1:]:
            value = value + one[at, :]
        return value

    @pl.loop(0, mine, unroll=8)
    def _(p):
        source_ref[p] = summed(proposals[0, offset + p] - first)

    side = lax.axis_index("row") & 1
    for rows, parity in ((kept_ref, side), (sent_ref, 1 - side)):

        @pl.loop(0, rows.shape[0], unroll=8)
        def _(q):
            block = lax.div(q, mine)
            row = proposals[1, (block + parity) * mine + q] - first
            here = (row >= 0) & (row < rows_tile)
            rows[q] = summed(jnp.where(here, row, 0)) * jnp.where(here, 1.0, 0.0)

    picked = [
        pltpu.make_async_copy(here, there, sem_rows.at[n])
        for n, (here, there) in enumerate(
            ((source_ref, source_rows), (kept_ref, kept_rows), (sent_ref, sent_rows))
        )
    ]
    for copy in picked:
        copy.start()
    chunk = total // 8
    for n in range(8):

        @pl.loop(0, chunk // 64)
        def _(i):
            at = pl.ds(pl.multiple_of(n * chunk + i * 64, 64), 64)
            value = main[at, :]
            for copy in copies:
                value = value + copy[at, :]
            main[at, :] = value

        at = pl.ds(n * chunk, chunk)
        pltpu.make_async_copy(main.at[at], out.at[at], sem_out).start()

    for copy in picked:
        copy.wait()
    pltpu.make_async_copy(main.at[pl.ds(0, total)], out, sem_out).wait()


def scatter(counts, arrived, proposals, capacity, row_devices):
    rows_tile, cols_tile = counts.shape
    cols_tiles = cols_tile // 128
    lines = counts.reshape(rows_tile // 8, 8, cols_tiles, 128).transpose(0, 2, 1, 3).reshape(-1, 128)
    total = lines.shape[0]
    count = proposals.shape[1]
    slots = (arrived.shape[0] * arrived.shape[2] // 128, 128)
    rows_shapes = [(size, cols_tiles, 128) for size in (count // row_devices, count // 2, count // 2)]
    out, source_rows, kept_rows, sent_rows = pl.pallas_call(
        functools.partial(scatter_kernel, capacity),
        out_shape=[jax.ShapeDtypeStruct(shape, jnp.float32) for shape in [lines.shape] + rows_shapes],
        in_specs=[
            pl.BlockSpec(memory_space=pltpu.VMEM),
            pl.BlockSpec(memory_space=pl.ANY),
            pl.BlockSpec(memory_space=pl.ANY),
        ],
        out_specs=[pl.BlockSpec(memory_space=pl.ANY)] * 4,
        scratch_shapes=[
            tuple(pltpu.VMEM((total + SPARE, 128), jnp.float32) for _ in range(COPIES - 1)),
            pltpu.VMEM((total + SPARE, 128), jnp.float32),
            pltpu.VMEM(slots, jnp.int32),
            pltpu.SMEM(slots, jnp.int32),
            pltpu.SMEM(proposals.shape, jnp.int32),
        ]
        + [pltpu.VMEM(shape, jnp.float32) for shape in rows_shapes]
        + [
            pltpu.SemaphoreType.DMA,
            pltpu.SemaphoreType.DMA,
            pltpu.SemaphoreType.DMA,
            pltpu.SemaphoreType.DMA((3,)),
            pltpu.SemaphoreType.DMA,
        ],
        compiler_params=pltpu.CompilerParams(vmem_limit_bytes=60000000),
        name="scatter",
    )(arrived, proposals, lines)
    updated = out.reshape(rows_tile // 8, cols_tiles, 8, 128).transpose(0, 2, 1, 3).reshape(rows_tile, cols_tile)
    return updated, source_rows, kept_rows, sent_rows


def terms_kernel(groups, cols_tile, proposals, own_ref, kept_ref, came_ref, out_ref):
    mine = own_ref.shape[0]
    per_col = mine // groups
    row_index = lax.axis_index("row")
    col_devices = lax.axis_size("col")
    shape = own_ref.shape[1:]
    position = (
        lax.axis_index("col") * cols_tile
        + 128 * lax.broadcasted_iota(jnp.int32, shape, 0)
        + lax.broadcasted_iota(jnp.int32, shape, 1)
    )
    zero = jnp.float32(0.0)
    lines = []
    for group in range(groups):
        columns = [[] for _ in range(6)]
        for k in range(per_col):
            p = group * per_col + k
            own = own_ref[p]
            other = kept_ref[p] + came_ref[p]
            at_source = position == proposals[0, row_index * mine + p]
            at_target = position == proposals[1, row_index * mine + p]
            mixed = entropy_term(own + other) - entropy_term(own) - entropy_term(other)
            values = (
                jnp.where(at_source | at_target, zero, mixed),
                jnp.where(at_source, own, zero),
                jnp.where(at_source, other, zero),
                jnp.where(at_target, other, zero),
                own,
                other,
            )
            for column, value in zip(columns, values):
                column.append(jnp.sum(value, axis=0, keepdims=True))
        rows = [row for column in columns for row in column]
        width = out_ref.shape[2]
        if len(rows) < width:
            rows.append(jnp.zeros((width - len(rows), 128), jnp.float32))
        lines.append(jnp.sum(jnp.concatenate(rows, axis=0).T, axis=0, keepdims=True))
    for device in range(out_ref.shape[0]):
        wanted, group = divmod(device % col_devices, groups)
        out_ref[device] = lines[group] * jnp.where(row_index == wanted, 1.0, 0.0)


def terms(proposals, own, kept, came, devices, cols_tile, per_col):
    width = -(-6 * per_col // 128) * 128
    return pl.pallas_call(
        functools.partial(terms_kernel, own.shape[0] // per_col, cols_tile),
        out_shape=jax.ShapeDtypeStruct((devices, 1, width), jnp.float32),
        in_specs=[pl.BlockSpec(memory_space=pltpu.SMEM)] + [pl.BlockSpec(memory_space=pltpu.VMEM)] * 3,
        out_specs=pl.BlockSpec(memory_space=pltpu.VMEM),
        name="terms",
    )(proposals, own, kept, came)


def per_device(counts, labels, edge_tiles, proposals, accept_flags):
    rows_tile, cols_tile = counts.shape
    row_devices = lax.axis_size("row")
    col_devices = lax.axis_size("col")
    devices = row_devices * col_devices
    edge_count = edge_tiles.shape[0] * edge_tiles.shape[2]
    capacity = 9 * edge_count // (2 * devices)
    slots = -(-capacity // 128) * 128
    outgoing = ingest(labels, edge_tiles, rows_tile, cols_tile, col_devices, devices, slots)
    arrived = lax.all_to_all(outgoing, ("row", "col"), split_axis=0, concat_axis=0, tiled=True)
    updated, own, kept, sent = scatter(counts, arrived, proposals, capacity, row_devices)

    mine = proposals.shape[1] // row_devices
    row_index = lax.axis_index("row")

    def swap(rows, bit):
        return lax.ppermute(rows, "row", [(device, device ^ (1 << bit)) for device in range(row_devices)])

    came = swap(sent, 0)
    for bit in range(1, log2_of(row_devices)):
        side = (row_index >> bit) & 1
        halves = (kept + came).reshape((-1, 2, mine) + kept.shape[1:])
        sent = lax.dynamic_index_in_dim(halves, 1 - side, 1, keepdims=False).reshape((-1,) + kept.shape[1:])
        kept = lax.dynamic_index_in_dim(halves, side, 1, keepdims=False).reshape((-1,) + kept.shape[1:])
        came = swap(sent, bit)
    per_col = accept_flags.shape[0]
    spread = terms(proposals, own, kept, came, devices, cols_tile, per_col)
    gathered = lax.all_to_all(spread, ("row", "col"), split_axis=0, concat_axis=0, tiled=True)
    sums = jnp.sum(gathered, axis=(0, 1))[: 6 * per_col].reshape(6, per_col)
    pair_sum, self_source, cross_count, self_target, degree_source, degree_target = sums
    corner = (
        entropy_term(self_source + 2.0 * cross_count + self_target)
        - entropy_term(self_source)
        - entropy_term(self_target)
        - 2.0 * entropy_term(cross_count)
    )
    change = (
        -(pair_sum + 0.5 * corner)
        + entropy_term(degree_source + degree_target)
        - entropy_term(degree_source)
        - entropy_term(degree_target)
    )
    merge_cost = change / (rows_tile * row_devices)
    accepted_cost = jnp.where(accept_flags == 1, merge_cost, jnp.float32(0.0))
    return (updated, merge_cost, accepted_cost)


def solution(mesh):
    return jax.shard_map(
        per_device,
        mesh=mesh,
        in_specs=(P("row", "col"), P(), P(("row", "col"), None, None), P(), P("col")),
        out_specs=(P("row", "col"), P("col"), P("col")),
        check_vma=False,
    )
```

```python
import functools

import jax
import jax.numpy as jnp
from jax import lax
from jax.experimental import pallas as pl
from jax.experimental.pallas import tpu as pltpu
from jax.sharding import PartitionSpec as P

COPIES = 6
GROUP = 8
SPARE = 32


def entropy_term(value):
    return value * jnp.log(jnp.maximum(value, 1.0))


def log2_of(size):
    assert size & (size - 1) == 0
    return size.bit_length() - 1


def ingest_kernel(
    rows_shift,
    cols_shift,
    col_shift,
    devices,
    ids_ref,
    table_hbm,
    out_ref,
    table_ref,
    lines_ref,
    lines_smem,
    picked,
    placed,
    sem_table,
    sem_lines,
):
    blocks = ids_ref.shape[0]
    slots = placed.shape[0]
    group = picked.shape[0] // 128
    rows_mask = (1 << rows_shift) - 1
    cols_mask = (1 << cols_shift) - 1

    def pick(index):
        for k in range(group):
            for lane in range(128):
                line = pl.ds(lines_smem[index * group + k, lane], 1)
                picked[k * 128 + lane : k * 128 + lane + 1, :] = table_ref[line, :]

    whole_table = pltpu.make_async_copy(table_hbm, table_ref, sem_table)
    whole_table.start()
    lines_ref[...] = ids_ref[...] >> 7
    lines = pltpu.make_async_copy(lines_ref, lines_smem, sem_lines)
    lines.start()
    placed[...] = jnp.zeros_like(placed)
    sublane = lax.broadcasted_iota(jnp.int32, (128, 128), 0)
    depth = lax.broadcasted_iota(jnp.int32, (128, 256), 0)
    width = lax.broadcasted_iota(jnp.int32, (128, 256), 1)
    upto = jnp.where((depth <= width) | (width >= 128), 1.0, 0.0).astype(jnp.bfloat16)
    owner_ids = lax.broadcasted_iota(jnp.int32, (devices, 128), 0)
    slot_ids = lax.broadcasted_iota(jnp.int32, (slots, 128), 0)
    steps = blocks // group
    lines.wait()
    whole_table.wait()
    pick(0)

    def place(index, carry, last=False):
        turned = [picked[k * 128 : (k + 1) * 128, :].T for k in range(group)]
        if not last:
            pick(index + 1)
        label = [
            jnp.sum(
                jnp.where(sublane == (ids_ref[pl.ds(index * group + k, 1), :] & 127), turned[k], 0),
                axis=0,
                keepdims=True,
            )
            for k in range(group)
        ]
        row = jnp.concatenate(label, axis=0)
        col = jnp.concatenate([label[k ^ 1] for k in range(group)], axis=0)
        owner = ((row >> rows_shift) << col_shift) + (col >> cols_shift)
        hot = [owner_ids == owner[k : k + 1, :] for k in range(group)]
        counted = jnp.dot(
            jnp.concatenate([jnp.where(h, 1.0, 0.0).astype(jnp.bfloat16) for h in hot], axis=0),
            upto,
            preferred_element_type=jnp.float32,
        )
        row_value = (row & rows_mask) + 1
        col_value = (col & cols_mask) + 1
        digits = [
            digit.astype(jnp.float32)
            for digit in (row_value >> 6, row_value & 63, col_value >> 6, col_value & 63)
        ]
        slot_parts = []
        digit_parts = []
        for k in range(group):
            part = counted[k * devices : (k + 1) * devices, :]
            rank = jnp.sum(jnp.where(hot[k], part[:, :128] + carry, 0.0), axis=0, keepdims=True)
            carry = carry + part[:, 128:]
            slot_parts.append(
                jnp.where(slot_ids == rank.astype(jnp.int32) - 1, 1.0, 0.0).astype(jnp.bfloat16)
            )
            digit_parts.append(
                jnp.concatenate(
                    [jnp.where(hot[k], d[k : k + 1, :], 0.0).astype(jnp.bfloat16) for d in digits],
                    axis=0,
                )
            )
        placed[...] += lax.dot_general(
            jnp.concatenate(slot_parts, axis=1),
            jnp.concatenate(digit_parts, axis=1),
            (((1,), (1,)), ((), ())),
            preferred_element_type=jnp.float32,
        )
        return carry

    place(steps - 1, lax.fori_loop(0, steps - 1, place, jnp.zeros((devices, 128), jnp.float32)), last=True)
    flat = placed[...].T.astype(jnp.int32)
    out_ref[:, 0, :] = flat[:devices] * 64 + flat[devices : 2 * devices] - 1
    out_ref[:, 1, :] = flat[2 * devices : 3 * devices] * 64 + flat[3 * devices :] - 1


def ingest(labels, edge_tiles, rows_tile, cols_tile, col_devices, devices, slots):
    ids = edge_tiles.reshape(-1, 128)
    table = labels.reshape(-1, 128)
    return pl.pallas_call(
        functools.partial(
            ingest_kernel, log2_of(rows_tile), log2_of(cols_tile), log2_of(col_devices), devices
        ),
        out_shape=jax.ShapeDtypeStruct((devices, 2, slots), jnp.int32),
        in_specs=[pl.BlockSpec(memory_space=pltpu.VMEM), pl.BlockSpec(memory_space=pl.ANY)],
        out_specs=pl.BlockSpec(memory_space=pltpu.VMEM),
        scratch_shapes=[
            pltpu.VMEM(table.shape, jnp.int32),
            pltpu.VMEM(ids.shape, jnp.int32),
            pltpu.SMEM(ids.shape, jnp.int32),
            pltpu.VMEM((GROUP * 128, 128), jnp.int32),
            pltpu.VMEM((slots, 4 * devices), jnp.float32),
            pltpu.SemaphoreType.DMA,
            pltpu.SemaphoreType.DMA,
        ],
        name="ingest",
    )(ids, table)


def scatter_kernel(
    capacity,
    arrived,
    proposals_hbm,
    counts,
    out,
    source_rows,
    kept_rows,
    sent_rows,
    copies,
    main,
    words_ref,
    lanes_ref,
    words,
    hot_ref,
    proposals,
    source_ref,
    kept_ref,
    sent_ref,
    sem_counts,
    sem_words,
    sem_proposals,
    sem_rows,
    sem_out,
):
    total = counts.shape[0]
    senders = arrived.shape[0]
    parts = arrived.shape[2] // 128
    cols_tiles = source_ref.shape[1]
    arrive = pltpu.make_async_copy(counts, main.at[pl.ds(0, total)], sem_counts)
    arrive.start()
    asked = pltpu.make_async_copy(proposals_hbm, proposals, sem_proposals)
    asked.start()
    spare = total + (lax.broadcasted_iota(jnp.int32, (senders, 128), 1) & (SPARE - 1))
    for part in range(parts):
        row = arrived[:, 0, part * 128 : (part + 1) * 128]
        col = arrived[:, 1, part * 128 : (part + 1) * 128]
        line = (((row >> 3) * cols_tiles + (col >> 7)) << 3) + (row & 7)
        at = pl.ds(part, senders, stride=parts)
        words_ref[at, :] = jnp.where(row >= 0, line, spare)
        lanes_ref[at, :] = col & 127
    listed = pltpu.make_async_copy(words_ref, words, sem_words)
    listed.start()
    zeros = jnp.zeros((256, 128), jnp.float32)
    for copy in copies:

        @pl.loop(0, total // 256)
        def _(i):
            copy[pl.ds(pl.multiple_of(i * 256, 256), 256), :] = zeros

    asked.wait()
    listed.wait()
    arrive.wait()
    sums = (main,) + tuple(copies)
    lane_ids = lax.broadcasted_iota(jnp.int32, (128, 128), 0)

    def hot_lines(at):
        return jnp.where(lane_ids == lanes_ref[pl.ds(at, 1), :], 1.0, 0.0).T

    def add_line(at, then, count):
        later = hot_lines(then)
        for slot in range(count):
            line = pl.ds(words[at, slot], 1)
            sums[slot % len(sums)][line, :] += hot_ref[slot : slot + 1, :]
        hot_ref[...] = later

    whole, rest = capacity // 128, capacity % 128
    hot_ref[...] = hot_lines(0)

    @pl.loop(0, senders)
    def _(sender):
        following = jnp.minimum(sender + 1, senders - 1) * parts
        if whole:

            @pl.loop(0, whole)
            def _(part):
                at = sender * parts + part
                then = at + 1 if rest else jnp.where(part == whole - 1, following, at + 1)
                add_line(at, then, 128)

        if rest:
            add_line(sender * parts + whole, following, rest)

    rows_tile = total // cols_tiles
    first = lax.axis_index("row") * rows_tile
    mine = source_ref.shape[0]
    offset = lax.axis_index("row") * mine

    def summed(row):
        at = pl.ds(((row >> 3) * cols_tiles << 3) + (row & 7), cols_tiles, stride=8)
        value = sums[0][at, :]
        for one in sums[1:]:
            value = value + one[at, :]
        return value

    @pl.loop(0, mine, unroll=8)
    def _(p):
        source_ref[p] = summed(proposals[0, offset + p] - first)

    side = lax.axis_index("row") & 1
    for rows, parity in ((kept_ref, side), (sent_ref, 1 - side)):

        @pl.loop(0, rows.shape[0], unroll=8)
        def _(q):
            block = lax.div(q, mine)
            row = proposals[1, (block + parity) * mine + q] - first
            here = (row >= 0) & (row < rows_tile)
            rows[q] = summed(jnp.where(here, row, 0)) * jnp.where(here, 1.0, 0.0)

    picked = [
        pltpu.make_async_copy(here, there, sem_rows.at[n])
        for n, (here, there) in enumerate(
            ((source_ref, source_rows), (kept_ref, kept_rows), (sent_ref, sent_rows))
        )
    ]
    for copy in picked:
        copy.start()
    chunk = total // 8
    for n in range(8):

        @pl.loop(0, chunk // 64)
        def _(i):
            at = pl.ds(pl.multiple_of(n * chunk + i * 64, 64), 64)
            value = main[at, :]
            for copy in copies:
                value = value + copy[at, :]
            main[at, :] = value

        at = pl.ds(n * chunk, chunk)
        pltpu.make_async_copy(main.at[at], out.at[at], sem_out).start()

    for copy in picked:
        copy.wait()
    pltpu.make_async_copy(main.at[pl.ds(0, total)], out, sem_out).wait()


def scatter(counts, arrived, proposals, capacity, row_devices):
    rows_tile, cols_tile = counts.shape
    cols_tiles = cols_tile // 128
    lines = counts.reshape(rows_tile // 8, 8, cols_tiles, 128).transpose(0, 2, 1, 3).reshape(-1, 128)
    total = lines.shape[0]
    count = proposals.shape[1]
    slots = (arrived.shape[0] * arrived.shape[2] // 128, 128)
    rows_shapes = [(size, cols_tiles, 128) for size in (count // row_devices, count // 2, count // 2)]
    out, source_rows, kept_rows, sent_rows = pl.pallas_call(
        functools.partial(scatter_kernel, capacity),
        out_shape=[jax.ShapeDtypeStruct(shape, jnp.float32) for shape in [lines.shape] + rows_shapes],
        in_specs=[
            pl.BlockSpec(memory_space=pltpu.VMEM),
            pl.BlockSpec(memory_space=pl.ANY),
            pl.BlockSpec(memory_space=pl.ANY),
        ],
        out_specs=[pl.BlockSpec(memory_space=pl.ANY)] * 4,
        scratch_shapes=[
            tuple(pltpu.VMEM((total + SPARE, 128), jnp.float32) for _ in range(COPIES - 1)),
            pltpu.VMEM((total + SPARE, 128), jnp.float32),
            pltpu.VMEM(slots, jnp.int32),
            pltpu.VMEM(slots, jnp.int32),
            pltpu.SMEM(slots, jnp.int32),
            pltpu.VMEM((128, 128), jnp.float32),
            pltpu.SMEM(proposals.shape, jnp.int32),
        ]
        + [pltpu.VMEM(shape, jnp.float32) for shape in rows_shapes]
        + [
            pltpu.SemaphoreType.DMA,
            pltpu.SemaphoreType.DMA,
            pltpu.SemaphoreType.DMA,
            pltpu.SemaphoreType.DMA((3,)),
            pltpu.SemaphoreType.DMA,
        ],
        compiler_params=pltpu.CompilerParams(vmem_limit_bytes=60000000),
        name="scatter",
    )(arrived, proposals, lines)
    updated = out.reshape(rows_tile // 8, cols_tiles, 8, 128).transpose(0, 2, 1, 3).reshape(rows_tile, cols_tile)
    return updated, source_rows, kept_rows, sent_rows


def terms_kernel(groups, cols_tile, proposals, own_ref, kept_ref, came_ref, out_ref):
    mine = own_ref.shape[0]
    per_col = mine // groups
    row_index = lax.axis_index("row")
    col_devices = lax.axis_size("col")
    shape = own_ref.shape[1:]
    position = (
        lax.axis_index("col") * cols_tile
        + 128 * lax.broadcasted_iota(jnp.int32, shape, 0)
        + lax.broadcasted_iota(jnp.int32, shape, 1)
    )
    zero = jnp.float32(0.0)
    lines = []
    for group in range(groups):
        columns = [[] for _ in range(6)]
        for k in range(per_col):
            p = group * per_col + k
            own = own_ref[p]
            other = kept_ref[p] + came_ref[p]
            at_source = position == proposals[0, row_index * mine + p]
            at_target = position == proposals[1, row_index * mine + p]
            mixed = entropy_term(own + other) - entropy_term(own) - entropy_term(other)
            values = (
                jnp.where(at_source | at_target, zero, mixed),
                jnp.where(at_source, own, zero),
                jnp.where(at_source, other, zero),
                jnp.where(at_target, other, zero),
                own,
                other,
            )
            for column, value in zip(columns, values):
                column.append(jnp.sum(value, axis=0, keepdims=True))
        rows = [row for column in columns for row in column]
        width = out_ref.shape[2]
        if len(rows) < width:
            rows.append(jnp.zeros((width - len(rows), 128), jnp.float32))
        lines.append(jnp.sum(jnp.concatenate(rows, axis=0).T, axis=0, keepdims=True))
    for device in range(out_ref.shape[0]):
        wanted, group = divmod(device % col_devices, groups)
        out_ref[device] = lines[group] * jnp.where(row_index == wanted, 1.0, 0.0)


def terms(proposals, own, kept, came, devices, cols_tile, per_col):
    width = -(-6 * per_col // 128) * 128
    return pl.pallas_call(
        functools.partial(terms_kernel, own.shape[0] // per_col, cols_tile),
        out_shape=jax.ShapeDtypeStruct((devices, 1, width), jnp.float32),
        in_specs=[pl.BlockSpec(memory_space=pltpu.SMEM)] + [pl.BlockSpec(memory_space=pltpu.VMEM)] * 3,
        out_specs=pl.BlockSpec(memory_space=pltpu.VMEM),
        name="terms",
    )(proposals, own, kept, came)


def per_device(counts, labels, edge_tiles, proposals, accept_flags):
    rows_tile, cols_tile = counts.shape
    row_devices = lax.axis_size("row")
    col_devices = lax.axis_size("col")
    devices = row_devices * col_devices
    edge_count = edge_tiles.shape[0] * edge_tiles.shape[2]
    capacity = 9 * edge_count // (2 * devices)
    slots = -(-capacity // 128) * 128
    outgoing = ingest(labels, edge_tiles, rows_tile, cols_tile, col_devices, devices, slots)
    arrived = lax.all_to_all(outgoing, ("row", "col"), split_axis=0, concat_axis=0, tiled=True)
    updated, own, kept, sent = scatter(counts, arrived, proposals, capacity, row_devices)

    mine = proposals.shape[1] // row_devices
    row_index = lax.axis_index("row")

    def swap(rows, bit):
        return lax.ppermute(rows, "row", [(device, device ^ (1 << bit)) for device in range(row_devices)])

    came = swap(sent, 0)
    for bit in range(1, log2_of(row_devices)):
        side = (row_index >> bit) & 1

        def half(rows, wanted):
            rows = rows.reshape((-1, 2, mine) + rows.shape[1:])
            rows = lax.dynamic_index_in_dim(rows, wanted, 1, keepdims=False)
            return rows.reshape((-1,) + rows.shape[2:])

        sent = half(kept, 1 - side) + half(came, 1 - side)
        kept = half(kept, side) + half(came, side)
        came = swap(sent, bit)
    per_col = accept_flags.shape[0]
    spread = terms(proposals, own, kept, came, devices, cols_tile, per_col)
    gathered = lax.all_to_all(spread, ("row", "col"), split_axis=0, concat_axis=0, tiled=True)
    sums = jnp.sum(gathered, axis=(0, 1))[: 6 * per_col].reshape(6, per_col)
    pair_sum, self_source, cross_count, self_target, degree_source, degree_target = sums
    corner = (
        entropy_term(self_source + 2.0 * cross_count + self_target)
        - entropy_term(self_source)
        - entropy_term(self_target)
        - 2.0 * entropy_term(cross_count)
    )
    change = (
        -(pair_sum + 0.5 * corner)
        + entropy_term(degree_source + degree_target)
        - entropy_term(degree_source)
        - entropy_term(degree_target)
    )
    merge_cost = change / (rows_tile * row_devices)
    accepted_cost = jnp.where(accept_flags == 1, merge_cost, jnp.float32(0.0))
    return (updated, merge_cost, accepted_cost)


def solution(mesh):
    return jax.shard_map(
        per_device,
        mesh=mesh,
        in_specs=(P("row", "col"), P(), P(("row", "col"), None, None), P(), P("col")),
        out_specs=(P("row", "col"), P("col"), P("col")),
        check_vma=False,
    )
```

```python
import functools

import jax
import jax.numpy as jnp
from jax import lax
from jax.experimental import pallas as pl
from jax.experimental.pallas import tpu as pltpu
from jax.sharding import PartitionSpec as P

COPIES = 6
GROUP = 8
SPARE = 32


def entropy_term(value):
    return value * jnp.log(jnp.maximum(value, 1.0))


def log2_of(size):
    assert size & (size - 1) == 0
    return size.bit_length() - 1


def ingest_kernel(
    rows_shift,
    cols_shift,
    col_shift,
    devices,
    ids_ref,
    table_hbm,
    out_ref,
    table_ref,
    lines_ref,
    lines_smem,
    picked,
    placed,
    sem_table,
    sem_lines,
):
    blocks = ids_ref.shape[0]
    slots = placed.shape[0]
    group = picked.shape[0] // 128
    rows_mask = (1 << rows_shift) - 1
    cols_mask = (1 << cols_shift) - 1

    def pick(index):
        for k in range(group):
            for lane in range(128):
                line = pl.ds(lines_smem[index * group + k, lane], 1)
                picked[k * 128 + lane : k * 128 + lane + 1, :] = table_ref[line, :]

    whole_table = pltpu.make_async_copy(table_hbm, table_ref, sem_table)
    whole_table.start()
    lines_ref[...] = ids_ref[...] >> 7
    lines = pltpu.make_async_copy(lines_ref, lines_smem, sem_lines)
    lines.start()
    placed[...] = jnp.zeros_like(placed)
    sublane = lax.broadcasted_iota(jnp.int32, (128, 128), 0)
    depth = lax.broadcasted_iota(jnp.int32, (128, 256), 0)
    width = lax.broadcasted_iota(jnp.int32, (128, 256), 1)
    upto = jnp.where((depth <= width) | (width >= 128), 1.0, 0.0).astype(jnp.bfloat16)
    owner_ids = lax.broadcasted_iota(jnp.int32, (devices, 128), 0)
    slot_ids = lax.broadcasted_iota(jnp.int32, (slots, 128), 0)
    steps = blocks // group
    lines.wait()
    whole_table.wait()
    pick(0)

    def place(index, carry, last=False):
        turned = [picked[k * 128 : (k + 1) * 128, :].T for k in range(group)]
        if not last:
            pick(index + 1)
        label = [
            jnp.sum(
                jnp.where(sublane == (ids_ref[pl.ds(index * group + k, 1), :] & 127), turned[k], 0),
                axis=0,
                keepdims=True,
            )
            for k in range(group)
        ]
        row = jnp.concatenate(label, axis=0)
        col = jnp.concatenate([label[k ^ 1] for k in range(group)], axis=0)
        owner = ((row >> rows_shift) << col_shift) + (col >> cols_shift)
        hot = [owner_ids == owner[k : k + 1, :] for k in range(group)]
        counted = jnp.dot(
            jnp.concatenate([jnp.where(h, 1.0, 0.0).astype(jnp.bfloat16) for h in hot], axis=0),
            upto,
            preferred_element_type=jnp.float32,
        )
        row_value = (row & rows_mask) + 1
        col_value = (col & cols_mask) + 1
        digits = [
            digit.astype(jnp.float32)
            for digit in (row_value >> 6, row_value & 63, col_value >> 6, col_value & 63)
        ]
        slot_parts = []
        digit_parts = []
        for k in range(group):
            part = counted[k * devices : (k + 1) * devices, :]
            rank = jnp.sum(jnp.where(hot[k], part[:, :128] + carry, 0.0), axis=0, keepdims=True)
            carry = carry + part[:, 128:]
            slot_parts.append(
                jnp.where(slot_ids == rank.astype(jnp.int32) - 1, 1.0, 0.0).astype(jnp.bfloat16)
            )
            digit_parts.append(
                jnp.concatenate(
                    [jnp.where(hot[k], d[k : k + 1, :], 0.0).astype(jnp.bfloat16) for d in digits],
                    axis=0,
                )
            )
        placed[...] += lax.dot_general(
            jnp.concatenate(slot_parts, axis=1),
            jnp.concatenate(digit_parts, axis=1),
            (((1,), (1,)), ((), ())),
            preferred_element_type=jnp.float32,
        )
        return carry

    place(steps - 1, lax.fori_loop(0, steps - 1, place, jnp.zeros((devices, 128), jnp.float32)), last=True)
    flat = placed[...].T.astype(jnp.int32)
    out_ref[:, 0, :] = flat[:devices] * 64 + flat[devices : 2 * devices] - 1
    out_ref[:, 1, :] = flat[2 * devices : 3 * devices] * 64 + flat[3 * devices :] - 1


def ingest(labels, edge_tiles, rows_tile, cols_tile, col_devices, devices, slots):
    ids = edge_tiles.reshape(-1, 128)
    table = labels.reshape(-1, 128)
    return pl.pallas_call(
        functools.partial(
            ingest_kernel, log2_of(rows_tile), log2_of(cols_tile), log2_of(col_devices), devices
        ),
        out_shape=jax.ShapeDtypeStruct((devices, 2, slots), jnp.int32),
        in_specs=[pl.BlockSpec(memory_space=pltpu.VMEM), pl.BlockSpec(memory_space=pl.ANY)],
        out_specs=pl.BlockSpec(memory_space=pltpu.VMEM),
        scratch_shapes=[
            pltpu.VMEM(table.shape, jnp.int32),
            pltpu.VMEM(ids.shape, jnp.int32),
            pltpu.SMEM(ids.shape, jnp.int32),
            pltpu.VMEM((GROUP * 128, 128), jnp.int32),
            pltpu.VMEM((slots, 4 * devices), jnp.float32),
            pltpu.SemaphoreType.DMA,
            pltpu.SemaphoreType.DMA,
        ],
        name="ingest",
    )(ids, table)


def scatter_kernel(
    capacity,
    arrived,
    proposals_hbm,
    counts,
    out,
    source_rows,
    kept_rows,
    sent_rows,
    copies,
    main,
    words_ref,
    lanes_ref,
    words,
    hot_ref,
    proposals,
    source_ref,
    kept_ref,
    sent_ref,
    sem_counts,
    sem_words,
    sem_proposals,
    sem_rows,
    sem_out,
):
    total = counts.shape[0]
    senders = arrived.shape[0]
    parts = arrived.shape[2] // 128
    cols_tiles = source_ref.shape[1]
    arrive = pltpu.make_async_copy(counts, main.at[pl.ds(0, total)], sem_counts)
    arrive.start()
    asked = pltpu.make_async_copy(proposals_hbm, proposals, sem_proposals)
    asked.start()
    spare = total + (lax.broadcasted_iota(jnp.int32, (senders, 128), 1) & (SPARE - 1))
    for part in range(parts):
        row = arrived[:, 0, part * 128 : (part + 1) * 128]
        col = arrived[:, 1, part * 128 : (part + 1) * 128]
        line = (((row >> 3) * cols_tiles + (col >> 7)) << 3) + (row & 7)
        at = pl.ds(part, senders, stride=parts)
        words_ref[at, :] = jnp.where(row >= 0, line, spare)
        lanes_ref[at, :] = col & 127
    listed = pltpu.make_async_copy(words_ref, words, sem_words)
    listed.start()
    zeros = jnp.zeros((256, 128), jnp.float32)
    for copy in copies:

        @pl.loop(0, total // 256)
        def _(i):
            copy[pl.ds(pl.multiple_of(i * 256, 256), 256), :] = zeros

    asked.wait()
    listed.wait()
    arrive.wait()
    sums = (main,) + tuple(copies)
    lane_ids = lax.broadcasted_iota(jnp.int32, (128, 128), 0)

    def hot_lines(at):
        return jnp.where(lane_ids == lanes_ref[pl.ds(at, 1), :], 1.0, 0.0).T

    def add_line(at, then, count):
        later = hot_lines(then)
        for slot in range(count):
            line = pl.ds(words[at, slot], 1)
            sums[slot % len(sums)][line, :] += hot_ref[slot : slot + 1, :]
        hot_ref[...] = later

    whole, rest = capacity // 128, capacity % 128
    hot_ref[...] = hot_lines(0)

    @pl.loop(0, senders)
    def _(sender):
        following = jnp.minimum(sender + 1, senders - 1) * parts
        if whole:

            @pl.loop(0, whole)
            def _(part):
                at = sender * parts + part
                then = at + 1 if rest else jnp.where(part == whole - 1, following, at + 1)
                add_line(at, then, 128)

        if rest:
            add_line(sender * parts + whole, following, rest)

    rows_tile = total // cols_tiles
    first = lax.axis_index("row") * rows_tile
    mine = source_ref.shape[0]
    offset = lax.axis_index("row") * mine

    def summed(row):
        at = pl.ds(((row >> 3) * cols_tiles << 3) + (row & 7), cols_tiles, stride=8)
        value = sums[0][at, :]
        for one in sums[1:]:
            value = value + one[at, :]
        return value

    @pl.loop(0, mine, unroll=16)
    def _(p):
        source_ref[p] = summed(proposals[0, offset + p] - first)

    side = lax.axis_index("row") & 1
    for rows, parity in ((kept_ref, side), (sent_ref, 1 - side)):

        @pl.loop(0, rows.shape[0], unroll=16)
        def _(q):
            block = lax.div(q, mine)
            row = proposals[1, (block + parity) * mine + q] - first
            here = (row >= 0) & (row < rows_tile)
            rows[q] = summed(jnp.where(here, row, 0)) * jnp.where(here, 1.0, 0.0)

    picked = [
        pltpu.make_async_copy(here, there, sem_rows.at[n])
        for n, (here, there) in enumerate(
            ((source_ref, source_rows), (kept_ref, kept_rows), (sent_ref, sent_rows))
        )
    ]
    for copy in picked:
        copy.start()
    chunk = total // 8
    for n in range(8):

        @pl.loop(0, chunk // 64)
        def _(i):
            at = pl.ds(pl.multiple_of(n * chunk + i * 64, 64), 64)
            value = main[at, :]
            for copy in copies:
                value = value + copy[at, :]
            main[at, :] = value

        at = pl.ds(n * chunk, chunk)
        pltpu.make_async_copy(main.at[at], out.at[at], sem_out).start()

    for copy in picked:
        copy.wait()
    pltpu.make_async_copy(main.at[pl.ds(0, total)], out, sem_out).wait()


def scatter(counts, arrived, proposals, capacity, row_devices):
    rows_tile, cols_tile = counts.shape
    cols_tiles = cols_tile // 128
    lines = counts.reshape(rows_tile // 8, 8, cols_tiles, 128).transpose(0, 2, 1, 3).reshape(-1, 128)
    total = lines.shape[0]
    count = proposals.shape[1]
    slots = (arrived.shape[0] * arrived.shape[2] // 128, 128)
    rows_shapes = [(size, cols_tiles, 128) for size in (count // row_devices, count // 2, count // 2)]
    out, source_rows, kept_rows, sent_rows = pl.pallas_call(
        functools.partial(scatter_kernel, capacity),
        out_shape=[jax.ShapeDtypeStruct(shape, jnp.float32) for shape in [lines.shape] + rows_shapes],
        in_specs=[
            pl.BlockSpec(memory_space=pltpu.VMEM),
            pl.BlockSpec(memory_space=pl.ANY),
            pl.BlockSpec(memory_space=pl.ANY),
        ],
        out_specs=[pl.BlockSpec(memory_space=pl.ANY)] * 4,
        scratch_shapes=[
            tuple(pltpu.VMEM((total + SPARE, 128), jnp.float32) for _ in range(COPIES - 1)),
            pltpu.VMEM((total + SPARE, 128), jnp.float32),
            pltpu.VMEM(slots, jnp.int32),
            pltpu.VMEM(slots, jnp.int32),
            pltpu.SMEM(slots, jnp.int32),
            pltpu.VMEM((128, 128), jnp.float32),
            pltpu.SMEM(proposals.shape, jnp.int32),
        ]
        + [pltpu.VMEM(shape, jnp.float32) for shape in rows_shapes]
        + [
            pltpu.SemaphoreType.DMA,
            pltpu.SemaphoreType.DMA,
            pltpu.SemaphoreType.DMA,
            pltpu.SemaphoreType.DMA((3,)),
            pltpu.SemaphoreType.DMA,
        ],
        compiler_params=pltpu.CompilerParams(vmem_limit_bytes=60000000),
        name="scatter",
    )(arrived, proposals, lines)
    updated = out.reshape(rows_tile // 8, cols_tiles, 8, 128).transpose(0, 2, 1, 3).reshape(rows_tile, cols_tile)
    return updated, source_rows, kept_rows, sent_rows


def terms_kernel(
    groups,
    cols_tile,
    proposals_hbm,
    own_hbm,
    kept_hbm,
    first_hbm,
    last_hbm,
    out_ref,
    proposals,
    own_ref,
    kept_ref,
    first_ref,
    last_ref,
    sems,
):
    top = log2_of(lax.axis_size("row")) - 1
    half = pl.ds(((lax.axis_index("row") >> top) & 1) * own_ref.shape[0], own_ref.shape[0])
    copies = [
        pltpu.make_async_copy(there, here, sems.at[n])
        for n, (there, here) in enumerate(
            (
                (proposals_hbm, proposals),
                (own_hbm, own_ref),
                (kept_hbm.at[half], kept_ref),
                (first_hbm.at[half], first_ref),
                (last_hbm, last_ref),
            )
        )
    ]
    for copy in copies:
        copy.start()
    for copy in copies:
        copy.wait()
    mine = own_ref.shape[0]
    per_col = mine // groups
    row_index = lax.axis_index("row")
    col_devices = lax.axis_size("col")
    shape = own_ref.shape[1:]
    position = (
        lax.axis_index("col") * cols_tile
        + 128 * lax.broadcasted_iota(jnp.int32, shape, 0)
        + lax.broadcasted_iota(jnp.int32, shape, 1)
    )
    zero = jnp.float32(0.0)
    lines = []
    for group in range(groups):
        columns = [[] for _ in range(6)]
        for k in range(per_col):
            p = group * per_col + k
            own = own_ref[p]
            other = kept_ref[p] + first_ref[p] + last_ref[p]
            at_source = position == proposals[0, row_index * mine + p]
            at_target = position == proposals[1, row_index * mine + p]
            mixed = entropy_term(own + other) - entropy_term(own) - entropy_term(other)
            values = (
                jnp.where(at_source | at_target, zero, mixed),
                jnp.where(at_source, own, zero),
                jnp.where(at_source, other, zero),
                jnp.where(at_target, other, zero),
                own,
                other,
            )
            for column, value in zip(columns, values):
                column.append(jnp.sum(value, axis=0, keepdims=True))
        rows = [row for column in columns for row in column]
        width = out_ref.shape[2]
        if len(rows) < width:
            rows.append(jnp.zeros((width - len(rows), 128), jnp.float32))
        lines.append(jnp.sum(jnp.concatenate(rows, axis=0).T, axis=0, keepdims=True))
    for device in range(out_ref.shape[0]):
        wanted, group = divmod(device % col_devices, groups)
        out_ref[device] = lines[group] * jnp.where(row_index == wanted, 1.0, 0.0)


def terms(proposals, own, kept, first, last, devices, cols_tile, per_col):
    width = -(-6 * per_col // 128) * 128
    return pl.pallas_call(
        functools.partial(terms_kernel, own.shape[0] // per_col, cols_tile),
        out_shape=jax.ShapeDtypeStruct((devices, 1, width), jnp.float32),
        in_specs=[pl.BlockSpec(memory_space=pl.ANY)] * 5,
        out_specs=pl.BlockSpec(memory_space=pltpu.VMEM),
        scratch_shapes=[pltpu.SMEM(proposals.shape, jnp.int32)]
        + [pltpu.VMEM(own.shape, jnp.float32)] * 4
        + [pltpu.SemaphoreType.DMA((5,))],
        compiler_params=pltpu.CompilerParams(vmem_limit_bytes=8 << 20),
        name="terms",
    )(proposals, own, kept, first, last)


def per_device(counts, labels, edge_tiles, proposals, accept_flags):
    rows_tile, cols_tile = counts.shape
    row_devices = lax.axis_size("row")
    col_devices = lax.axis_size("col")
    devices = row_devices * col_devices
    edge_count = edge_tiles.shape[0] * edge_tiles.shape[2]
    capacity = 9 * edge_count // (2 * devices)
    slots = -(-capacity // 128) * 128
    outgoing = ingest(labels, edge_tiles, rows_tile, cols_tile, col_devices, devices, slots)
    arrived = lax.all_to_all(outgoing, ("row", "col"), split_axis=0, concat_axis=0, tiled=True)
    updated, own, kept, sent = scatter(counts, arrived, proposals, capacity, row_devices)

    mine = proposals.shape[1] // row_devices
    row_index = lax.axis_index("row")

    def swap(rows, bit):
        return lax.ppermute(rows, "row", [(device, device ^ (1 << bit)) for device in range(row_devices)])

    def half(rows, wanted):
        rows = rows.reshape((-1, 2, mine) + rows.shape[1:])
        rows = lax.dynamic_index_in_dim(rows, wanted, 1, keepdims=False)
        return rows.reshape((-1,) + rows.shape[2:])

    bits = log2_of(row_devices)
    assert bits > 1
    came = swap(sent, 0)
    for bit in range(1, bits - 1):
        side = (row_index >> bit) & 1
        sent = half(kept, 1 - side) + half(came, 1 - side)
        kept = half(kept, side) + half(came, side)
        came = swap(sent, bit)
    side = (row_index >> (bits - 1)) & 1
    last = swap(half(kept, 1 - side) + half(came, 1 - side), bits - 1)
    per_col = accept_flags.shape[0]
    spread = terms(proposals, own, kept, came, last, devices, cols_tile, per_col)
    gathered = lax.all_to_all(spread, ("row", "col"), split_axis=0, concat_axis=0, tiled=True)
    sums = jnp.sum(gathered, axis=(0, 1))[: 6 * per_col].reshape(6, per_col)
    pair_sum, self_source, cross_count, self_target, degree_source, degree_target = sums
    corner = (
        entropy_term(self_source + 2.0 * cross_count + self_target)
        - entropy_term(self_source)
        - entropy_term(self_target)
        - 2.0 * entropy_term(cross_count)
    )
    change = (
        -(pair_sum + 0.5 * corner)
        + entropy_term(degree_source + degree_target)
        - entropy_term(degree_source)
        - entropy_term(degree_target)
    )
    merge_cost = change / (rows_tile * row_devices)
    accepted_cost = jnp.where(accept_flags == 1, merge_cost, jnp.float32(0.0))
    return (updated, merge_cost, accepted_cost)


def solution(mesh):
    return jax.shard_map(
        per_device,
        mesh=mesh,
        in_specs=(P("row", "col"), P(), P(("row", "col"), None, None), P(), P("col")),
        out_specs=(P("row", "col"), P("col"), P("col")),
        check_vma=False,
    )
```
